32 devices in a mesh: cell: 16 (over z, y, x), view: 2 (over core).
Axes of the slice: x: 2, y: 2, z: 4, core: 2. Of those that a mesh axis runs over, the one named last changes fastest.
Arguments:
- params: float32 [7, 131072], P(None, 'cell'), may hold values from -4.5 to 4.5
- first_moment: float32 [7, 131072], P(None, 'cell'), may hold values from -6e-05 to 6e-05
- second_moment: float32 [7, 131072], P(None, 'cell'), may hold values from 1e-11 to 1e-08
- camera: float32 [1, 2, 4], P(None, 'view'), may hold values from -0.3 to 0.3
- slot_block: int32 [1, 2, 16, 16, 4], P(None, 'view', 'cell'), may hold values from -1 to 63, as said below
- slot_anchor: float32 [1, 2, 16, 2, 16, 4], P(None, 'view', 'cell'), may hold values from -0.3 to 0.3
- tile_items: int32 [1, 2, 128, 4], P(None, 'view', 'cell'), may hold values from 0 to 63, as said below
- target: float32 [1, 2, 128, 3, 256], P(None, 'view', 'cell'), may hold values from 0 to 1
Outputs:
- new_params: float32 [7, 131072], P(None, 'cell')
- tile_loss: float32 [1, 2, 128], P(None, 'view', 'cell')
The draws below stay inside these ranges and needn't reach their ends.
Inputs may be any that keep to these rules, and one draw needn't show every extreme that they name: `slot_block`: -1 marks an empty slot; in every step and view each owner receives all 4 slots from some cell. `tile_items`: entry c * 4 + j names the live slot j from cell c to the tile's owner (tile // 8); every live slot is named exactly once, and the 4 entries of a tile come from distinct cells.
All inputs are finite; a program needn't handle non-finite values.
Results may differ from the reference program's by a relative error of at most 0.00035.
Values sent between devices are 32-bit elements; how exact they have to be, the bound alone decides.
No kernel may reach another device: no remote copies, remote signals or barrier semaphores. Data moves between devices by JAX's collectives and lax.ppermute only.
A program may use at most 64 MiB of HBM per device.

```python
import math
import jax
import jax.numpy as jnp
import numpy as np
from jax import lax

SIDE = 16
PIX = 256
BLOCK = 128
PARAMS = 7
TAPS = 11
DEPTH = 4
STEPS = 1
TILE_DEV = 8
BLOCKS_DEV = 64
CAP = 4
VIEWS = 2
TILES = 128
GAUSS = 131072
N_CELL = 16


def routing_tables(key):
    base_key = jax.random.fold_in(key, 7177)
    number_of_slots = N_CELL * CAP
    item_count = TILE_DEV * DEPTH

    def one_view(view_key):
        heat_key, rest_key = jax.random.split(view_key)
        warmth_level = jax.random.randint(heat_key, (N_CELL,), 0, 8) ** 2

        def one_owner(owner_key):
            sub_keys = jax.random.split(owner_key, 5)
            warmest_entry = jax.random.randint(sub_keys[0], (), 0, N_CELL)
            extra_warmth = jnp.where(jnp.arange(N_CELL) == warmest_entry, 1000, 0)
            source_items = jnp.arange(number_of_slots) // CAP
            random_noise = jax.random.randint(sub_keys[1], (number_of_slots,), 0, 4096)
            score_values = ((warmth_level + extra_warmth)[source_items] * 1024 + random_noise) * number_of_slots + jnp.arange(number_of_slots)
            unused_values, chosen = lax.top_k(score_values, item_count)
            chosen = jnp.sort(chosen)
            columns = chosen.reshape(DEPTH, TILE_DEV).T
            depth_keys = jax.random.split(sub_keys[2], TILE_DEV)
            orders = jax.vmap(lambda row_key: jax.random.permutation(row_key, DEPTH))(depth_keys)
            columns = jnp.take_along_axis(columns, orders, axis=1)
            tile_order = jax.random.permutation(sub_keys[3], TILE_DEV)
            columns = columns[tile_order]
            used_flags = jnp.zeros((number_of_slots,), jnp.int32).at[chosen].set(1)
            block_ids = jax.random.randint(sub_keys[4], (number_of_slots,), 0, BLOCKS_DEV)
            slot_table = jnp.where(used_flags > 0, block_ids, -1).reshape(N_CELL, CAP)
            return (slot_table, columns)
        owner_keys = jax.random.split(rest_key, N_CELL)
        slot_table, columns = jax.vmap(one_owner)(owner_keys)
        return (jnp.transpose(slot_table, (1, 0, 2)), columns.reshape(N_CELL * TILE_DEV, DEPTH))
    view_keys = jax.random.split(base_key, STEPS * VIEWS)
    slot_table, columns = jax.vmap(one_view)(view_keys)
    return (slot_table.reshape(STEPS, VIEWS, N_CELL, N_CELL, CAP), columns.reshape(STEPS, VIEWS, TILES, DEPTH))


def draw_slot_block(key, part):
    return routing_tables(key)[0].astype(jnp.int32)


def draw_tile_items(key, part):
    return routing_tables(key)[1].astype(jnp.int32)


def draw_params(key, part):
    sub_keys = jax.random.split(jax.random.fold_in(key, 31), 4)
    count = GAUSS
    place_xy = jax.random.uniform(sub_keys[0], (2, count), jnp.float32, 0.0, 1.0)
    log_scale = jax.random.uniform(sub_keys[1], (1, count), jnp.float32, -3.0, -1.6)
    opacity_logit = jnp.clip(1.5 * jax.random.normal(sub_keys[2], (1, count), jnp.float32), -4.5, 4.5)
    colour_logit = jnp.clip(1.5 * jax.random.normal(sub_keys[3], (3, count), jnp.float32), -4.5, 4.5)
    return jnp.concatenate([place_xy, log_scale, opacity_logit, colour_logit], axis=0)


def steps_of(rng, extent, cuts, low, top_value):
    def one(position, shards_of):
        heights = jax.random.uniform(jax.random.fold_in(jax.random.fold_in(rng, 6), position), (shards_of,), jnp.float32, low / len(cuts), top_value / len(cuts))
        return jnp.repeat(jnp.exp(heights), extent[position] // shards_of).reshape((-1,) + (1,) * (len(extent) - position - 1))

    gain = one(*cuts[0])
    for cut in cuts[1:]:
        gain = gain * one(*cut)
    return gain


def bell_draw(key, shape, deviation, reach, cuts=(), held_as=jnp.bfloat16):
    array = deviation * jax.random.normal(key, shape, jnp.float32)
    if cuts:
        array = array * steps_of(key, shape, cuts, -0.22, 0.18)
    return jnp.clip(array, -reach, reach).astype(held_as)


def setup_inputs(seed: int = 0) -> dict:
    streams_of = jax.random.split(jax.random.key(seed), 9)
    params = draw_params(jax.random.fold_in(streams_of[8], 71), 0)
    first_moment = bell_draw(streams_of[1], (PARAMS, GAUSS), 0.00001, 5.999999848427251e-05, ((1, 16),), jnp.float32)
    second_moment = jnp.clip(jnp.exp(math.log(9.99999993922529e-09) - 6.9077553 * jax.random.uniform(streams_of[2], (PARAMS, GAUSS), jnp.float32) ** steps_of(streams_of[2], (PARAMS, GAUSS), ((1, 16),), -0.2, 0.2)), 9.999999960041972e-12, 9.99999993922529e-09)
    camera = jnp.clip(jax.random.uniform(streams_of[3], (STEPS, VIEWS, 4), jnp.float32, -0.3, 0.3) * steps_of(streams_of[3], (STEPS, VIEWS, 4), ((1, 2),), -0.4, 0.0), -0.3, 0.3)
    slot_block = draw_slot_block(jax.random.fold_in(streams_of[8], 71), 0)
    slot_anchor = jnp.clip(jax.random.uniform(streams_of[5], (STEPS, VIEWS, N_CELL, 2, N_CELL, CAP), jnp.float32, -0.3, 0.3) * steps_of(streams_of[5], (STEPS, VIEWS, N_CELL, 2, N_CELL, CAP), ((1, 2), (2, 16)), -0.4, 0.0), -0.3, 0.3)
    tile_items = draw_tile_items(jax.random.fold_in(streams_of[8], 71), 0)
    target = jnp.clip(1.0 * jax.random.uniform(streams_of[7], (STEPS, VIEWS, TILES, 3, PIX), jnp.float32) ** steps_of(streams_of[7], (STEPS, VIEWS, TILES, 3, PIX), ((1, 2), (2, 16)), -0.2, 0.2), 0.0, 1.0)
    return dict(params=params, first_moment=first_moment, second_moment=second_moment, camera=camera, slot_block=slot_block, slot_anchor=slot_anchor, tile_items=tile_items, target=target)


ssim_weight = 0.2
stable_one = 0.0001
stable_two = 0.0009
learn_rate = 0.1
beta_one = 0.9
beta_two = 0.999
adam_eps = 1e-08
first_step = 1
opacity_cap = 0.1
weight_floor = 0.5
highest = lax.Precision.HIGHEST

def blur_matrix(tile_side, taps_count):
    offsets = np.arange(tile_side)[:, None] - np.arange(tile_side)[None, :]
    kernel = np.exp(-(offsets * offsets) / 4.5) * (np.abs(offsets) <= taps_count // 2)
    kernel = kernel / kernel.sum(axis=1, keepdims=True)
    return jnp.asarray(np.kron(kernel, kernel).T, jnp.float32)

def pixel_grid(tile_side):
    places = jnp.arange(tile_side * tile_side, dtype=jnp.int32)
    grid_x = ((places % tile_side).astype(jnp.float32) + 0.5) / tile_side
    grid_y = ((places // tile_side).astype(jnp.float32) + 0.5) / tile_side
    return (grid_x, grid_y)

def splat_block(block_params, camera_row, anchors, grid_x, grid_y):
    pos_x = block_params[:, 0]
    pos_y = block_params[:, 1]
    mean_u = (1.0 + camera_row[0]) * pos_x + camera_row[1] * pos_y + anchors[:, 0:1]
    mean_w = camera_row[2] * pos_x + (1.0 + camera_row[3]) * pos_y + anchors[:, 1:2]
    inverse = 0.5 * jnp.exp(-2.0 * block_params[:, 2])
    opacity = opacity_cap * jax.nn.sigmoid(block_params[:, 3])
    colours = jax.nn.sigmoid(block_params[:, 4:7])
    delta_x = grid_x[None, None, :] - mean_u[:, :, None]
    delta_y = grid_y[None, None, :] - mean_w[:, :, None]
    alphas = opacity[:, :, None] * jnp.exp(-(delta_x * delta_x + delta_y * delta_y) * inverse[:, :, None])
    weighted = jnp.einsum('ncg,ngp->ncp', colours, alphas, precision=highest)
    totals = lax.optimization_barrier(jnp.sum(alphas, axis=1))
    transmit = jnp.exp(lax.optimization_barrier(jnp.sum(jnp.log1p(-alphas), axis=1)))
    shaded = (1.0 - transmit)[:, None, :] * weighted / jnp.maximum(totals, weight_floor)[:, None, :]
    return jnp.concatenate([shaded, transmit[:, None, :]], axis=1)

def merge_tiles(items):
    fronts = jnp.ones_like(items[:, 0, 3])
    images = jnp.zeros_like(items[:, 0, :3])
    for rank_index in range(items.shape[1]):
        images = images + fronts[:, None, :] * items[:, rank_index, :3]
        fronts = fronts * items[:, rank_index, 3]
    return images

def tile_losses(images, goal_tiles, blur_table):
    tile_count = images.shape[0]
    predicted = images.reshape(tile_count * 3, -1)
    wanted = goal_tiles.reshape(tile_count * 3, -1)
    stacked = jnp.concatenate([predicted, wanted, predicted * predicted, wanted * wanted, predicted * wanted], axis=0)
    blurred = jnp.dot(stacked, blur_table, precision=highest, preferred_element_type=jnp.float32)
    local_pred, local_goal, square_pred, square_goal, cross_term = jnp.split(blurred, 5, axis=0)
    var_pred = square_pred - local_pred * local_pred
    var_goal = square_goal - local_goal * local_goal
    cov_both = cross_term - local_pred * local_goal
    similar = (2.0 * local_pred * local_goal + stable_one) * (2.0 * cov_both + stable_two) / ((local_pred * local_pred + local_goal * local_goal + stable_one) * (var_pred + var_goal + stable_two))
    residue = predicted - wanted
    values = (1.0 - ssim_weight) * residue * residue + ssim_weight * (1.0 - similar)
    return lax.optimization_barrier(jnp.mean(values.reshape(tile_count, -1), axis=1))

def reference(params, first_moment, second_moment, camera, slot_block, slot_anchor, tile_items, target):
    blur_table = blur_matrix(SIDE, TAPS)
    grid_x, grid_y = pixel_grid(SIDE)
    per_cell = BLOCKS_DEV * BLOCK
    lane_ids = jnp.arange(BLOCK, dtype=jnp.int32)
    owners = jnp.arange(N_CELL, dtype=jnp.int32)
    current = params
    moment_one = first_moment
    moment_two = second_moment
    loss_rows = []
    for step_index in range(STEPS):

        def view_step(summed, view_data):
            camera_row, blocks_view, anchors_view, items_view, goals_view = view_data

            def owner_pass(gradient, owner_id):
                entries = lax.dynamic_slice_in_dim(items_view, owner_id * TILE_DEV, TILE_DEV, 0).reshape(-1)
                source_items = entries // CAP
                slot_id = entries % CAP
                block_id = blocks_view[source_items, owner_id, slot_id]
                anchors = anchors_view[source_items, :, owner_id, slot_id]
                gauss_index = (source_items * per_cell + block_id * BLOCK)[:, None] + lane_ids[None, :]
                item_params = jnp.transpose(current[:, gauss_index], (1, 0, 2))
                goal_tiles = lax.dynamic_slice_in_dim(goals_view, owner_id * TILE_DEV, TILE_DEV, 0)

                def owner_loss(inner_params):
                    partial_value = splat_block(inner_params, camera_row, anchors, grid_x, grid_y)
                    return tile_losses(merge_tiles(partial_value.reshape(TILE_DEV, DEPTH, 4, PIX)), goal_tiles, blur_table)
                losses, pullback = jax.vjp(owner_loss, item_params)
                item_grads = pullback(jnp.ones_like(losses))[0]
                gradient = gradient.at[:, gauss_index].add(jnp.transpose(item_grads, (1, 0, 2)))
                return (gradient, losses)
            gradient, losses = lax.scan(owner_pass, jnp.zeros_like(current), owners)
            return (summed + gradient, losses.reshape(-1))
        gradient, losses = lax.scan(view_step, jnp.zeros_like(current), (camera[step_index], slot_block[step_index], slot_anchor[step_index], tile_items[step_index], target[step_index]))
        loss_rows.append(losses)
        step_count = first_step + step_index
        fix_one = 1.0 - beta_one ** step_count
        fix_two = 1.0 - beta_two ** step_count
        moment_one = beta_one * moment_one + (1.0 - beta_one) * gradient
        moment_two = beta_two * moment_two + (1.0 - beta_two) * gradient * gradient
        current = current - learn_rate * (moment_one / fix_one) / (jnp.sqrt(moment_two / fix_two) + adam_eps)
    return (current, jnp.stack(loss_rows))
```

```python
import functools

import jax
import jax.numpy as jnp
import numpy as np
from jax import lax
from jax.experimental import pallas as pl
from jax.experimental.pallas import tpu as pltpu
from jax.sharding import PartitionSpec as P

SIDE = 16
BLOCK = 128
TAPS = 11
PIX = SIDE * SIDE
ROWS = 8

ssim_weight = 0.2
stable_one = 0.0001
stable_two = 0.0009
learn_rate = 0.1
beta_one = 0.9
beta_two = 0.999
adam_eps = 1e-08
first_step = 1
opacity_cap = 0.1
weight_floor = 0.5
highest = lax.Precision.HIGHEST
f32 = jnp.float32
bf16 = jnp.bfloat16
CHUNK = 16

vmem = pl.BlockSpec(memory_space=pltpu.VMEM)
smem = pl.BlockSpec(memory_space=pltpu.SMEM)
anyspace = pl.BlockSpec(memory_space=pl.ANY)


def blur_kron():
    offsets = np.arange(SIDE)[:, None] - np.arange(SIDE)[None, :]
    kernel = np.exp(-(offsets * offsets) / 4.5) * (np.abs(offsets) <= TAPS // 2)
    kernel = kernel / kernel.sum(axis=1, keepdims=True)
    return np.kron(kernel, kernel).astype(np.float32)


def moment_basis():
    places = np.arange(PIX)
    x = (places % SIDE) - (SIDE - 1) / 2
    y = (places // SIDE) - (SIDE - 1) / 2
    rows = np.zeros((ROWS, PIX), np.float32)
    rows[0], rows[1], rows[2], rows[3], rows[4] = 1.0, x, y, x * x, y * y
    return rows


def pack_kernel(block_ref, anchor_ref, camera_ref, params_ref, out_ref):
    capacity, owners = block_ref.shape
    components = params_ref.shape[0]
    xx = 1.0 + camera_ref[0, 0]
    xy = camera_ref[0, 1]
    yx = camera_ref[0, 2]
    yy = 1.0 + camera_ref[0, 3]
    for owner in range(owners):
        for slot in range(capacity):
            block = jnp.maximum(block_ref[slot, owner], 0)
            lanes = pl.ds(pl.multiple_of(block * BLOCK, BLOCK), BLOCK)
            tile = params_ref[:, lanes]
            pos_x, pos_y = tile[0:1], tile[1:2]
            row = owner * capacity + slot
            out_ref[row, 0:1, :] = xx * pos_x + xy * pos_y + anchor_ref[0, slot, owner]
            out_ref[row, 1:2, :] = yx * pos_x + yy * pos_y + anchor_ref[1, slot, owner]
            out_ref[row, 2:components, :] = tile[2:]
            out_ref[row, components:, :] = jnp.zeros((ROWS - components, BLOCK), f32)


def split_pair(value):
    high = value.astype(bf16)
    return high, (value - high.astype(f32)).astype(bf16)


def owner_kernel(
    items_ref, camera_ref, arrived_ref, goal_ref, table_ref, basis_ref,
    back_ref, loss_ref,
    quant_ref, bcast_ref, alpha_ref, split_ref, part_ref, diff_ref, mix_ref, lhs_ref, rhs_ref,
):
    depth, tiles = items_ref.shape
    channels = goal_ref.shape[0]
    count = depth * tiles
    back_ref[...] = jnp.zeros_like(back_ref)
    lane = lax.broadcasted_iota(jnp.int32, (CHUNK, BLOCK), 1)
    grid_x = ((lane % SIDE).astype(f32) + 0.5) / SIDE
    grid_y = [((lane // SIDE + half * (BLOCK // SIDE)).astype(f32) + 0.5) / SIDE for half in range(2)]
    row8 = lax.broadcasted_iota(jnp.int32, (ROWS, BLOCK), 0)

    def quantities(index, carry):
        slot = items_ref[index // tiles, index % tiles]
        raw = arrived_ref[slot]
        sig = jax.nn.sigmoid(raw)
        spread = 0.5 * jnp.exp(-2.0 * raw)
        value = jnp.where(row8 < 2, raw, jnp.where(row8 == 2, spread, jnp.where(row8 == 3, opacity_cap * sig, sig)))
        quant_ref[index] = value
        columns = value.T
        for q in range(4):
            bcast_ref[q, index] = jnp.broadcast_to(columns[:, q : q + 1], (BLOCK, BLOCK))
        return carry

    lax.fori_loop(0, count, quantities, 0, unroll=4)

    def forward(index, carry):
        prods = [None, None]
        for chunk in range(BLOCK // CHUNK):
            part = pl.ds(chunk * CHUNK, CHUNK)
            mean_u, mean_w = bcast_ref[0, index, part, :], bcast_ref[1, index, part, :]
            inverse, opacity = bcast_ref[2, index, part, :], bcast_ref[3, index, part, :]
            delta_x = grid_x - mean_u
            square_x = delta_x * delta_x
            for half in range(2):
                delta_y = grid_y[half] - mean_w
                alpha = opacity * jnp.exp(-(square_x + delta_y * delta_y) * inverse)
                pixels = pl.ds(half * BLOCK, BLOCK)
                alpha_ref[index, part, pixels] = alpha
                high, low = split_pair(alpha)
                split_ref[index, part, pixels] = high
                split_ref[index, pl.ds(BLOCK + chunk * CHUNK, CHUNK), pixels] = low
                clear = 1.0 - alpha
                prods[half] = clear if prods[half] is None else prods[half] * clear
        clears = []
        for half in range(2):
            prod = prods[half][:ROWS] * prods[half][ROWS:]
            for shift in (4, 2, 1):
                prod = prod * pltpu.roll(prod, shift, 0)
            clears.append(prod[0:1])
        value = quant_ref[index]
        colour = jnp.where((row8 >= 4) & (row8 < 7), value, jnp.where(row8 == 7, 1.0, 0.0))
        high, low = split_pair(colour)
        low = jnp.where(row8 == 7, 0.0, low.astype(f32)).astype(bf16)
        left = jnp.concatenate([high, low], axis=0)
        right = jnp.concatenate([high, jnp.zeros_like(low)], axis=0)
        left = jnp.concatenate([left, right], axis=1)
        sums = jnp.dot(left, split_ref[index], preferred_element_type=f32)
        part_ref[index] = sums[:ROWS] + sums[ROWS:]
        for half in range(2):
            part_ref[index, 0:1, pl.ds(half * BLOCK, BLOCK)] = clears[half]
        return carry

    lax.fori_loop(0, count, forward, 0, unroll=2)

    def gathered(row, rank):
        return part_ref[rank * tiles : (rank + 1) * tiles, row, :]

    transmits = [gathered(0, rank) for rank in range(depth)]
    totals = [gathered(7, rank) for rank in range(depth)]
    floors = [jnp.maximum(total, weight_floor) for total in totals]
    ratios = [(1.0 - transmit) / floor for transmit, floor in zip(transmits, floors)]
    weighted = [[gathered(4 + ch, rank) for ch in range(channels)] for rank in range(depth)]
    shaded = [[ratios[rank] * weighted[rank][ch] for ch in range(channels)] for rank in range(depth)]
    fronts = [jnp.ones_like(transmits[0])]
    for rank in range(depth):
        fronts.append(fronts[rank] * transmits[rank])
    images = [sum(fronts[rank] * shaded[rank][ch] for rank in range(depth)) for ch in range(channels)]
    goals = [goal_ref[ch] for ch in range(channels)]
    image = jnp.concatenate(images, axis=0)
    goal = jnp.concatenate(goals, axis=0)
    stacked = jnp.concatenate([image, goal, image * image, goal * goal, image * goal], axis=0)
    blurred = lax.dot_general(stacked, table_ref[...], (((1,), (1,)), ((), ())), precision=highest, preferred_element_type=f32)
    size = channels * tiles
    local_a, local_b, square_a, square_b, cross = [blurred[i * size : (i + 1) * size] for i in range(5)]
    var_a = square_a - local_a * local_a
    var_b = square_b - local_b * local_b
    both = cross - local_a * local_b
    top_one = 2.0 * local_a * local_b + stable_one
    top_two = 2.0 * both + stable_two
    low_one = local_a * local_a + local_b * local_b + stable_one
    low_two = var_a + var_b + stable_two
    under = 1.0 / (low_one * low_two)
    similar = top_one * top_two * under
    residue = image - goal
    values = (1.0 - ssim_weight) * residue * residue + ssim_weight * (1.0 - similar)
    per_tile = values[:tiles]
    for ch in range(1, channels):
        per_tile = per_tile + values[ch * tiles : (ch + 1) * tiles]
    norm = 1.0 / (channels * PIX)
    column = jnp.sum(per_tile, axis=1, keepdims=True) * norm
    loss_ref[...] = jnp.broadcast_to(column, (tiles, BLOCK)).T[0:1, :]
    scale = -ssim_weight * norm
    by_top_one = scale * top_two * under
    by_top_two = scale * top_one * under
    by_low_one = -scale * similar / low_one
    by_low_two = -scale * similar / low_two
    by_local = 2.0 * (local_b * (by_top_one - by_top_two) + local_a * (by_low_one - by_low_two))
    spread = jnp.dot(
        jnp.concatenate([by_local, by_low_two, 2.0 * by_top_two], axis=0),
        table_ref[...], precision=highest, preferred_element_type=f32,
    )
    by_image = (
        (2.0 * (1.0 - ssim_weight) * norm) * residue
        + spread[:size] + 2.0 * image * spread[size : 2 * size] + goal * spread[2 * size :]
    )
    by_image = [by_image[ch * tiles : (ch + 1) * tiles] for ch in range(channels)]
    diff_ref[...] = jnp.zeros_like(diff_ref)

    def spread_rows(row, rank, value):
        diff_ref[rank * tiles : (rank + 1) * tiles, row, :] = value

    by_front = None
    for rank in reversed(range(depth)):
        by_shaded = [fronts[rank] * by_image[ch] for ch in range(channels)]
        by_transmit = -sum(by_shaded[ch] * weighted[rank][ch] for ch in range(channels)) / floors[rank]
        if by_front is not None:
            by_transmit = by_transmit + by_front * fronts[rank]
        own = sum(by_image[ch] * shaded[rank][ch] for ch in range(channels))
        by_front = own if by_front is None else own + by_front * transmits[rank]
        by_floor = -sum(by_shaded[ch] * shaded[rank][ch] for ch in range(channels)) / floors[rank]
        total = totals[rank]
        by_total = by_floor * jnp.where(total > weight_floor, 1.0, jnp.where(total == weight_floor, 0.5, 0.0))
        for q in range(4):
            value = by_shaded[q] * ratios[rank] if q < channels else by_total
            high = value.astype(bf16).astype(f32)
            spread_rows(q, rank, high)
            spread_rows(4 + q, rank, value - high)
            if q < channels:
                spread_rows(8 + q, rank, high)
        spread_rows(11, rank, by_transmit * transmits[rank])

    rhs_ref[...] = jnp.zeros_like(rhs_ref)
    xx = 1.0 + camera_ref[0, 0]
    xy = camera_ref[0, 1]
    yx = camera_ref[0, 2]
    yy = 1.0 + camera_ref[0, 3]
    for block in range(2):
        rhs_ref[0:ROWS, pl.ds(block * PIX, PIX)] = basis_ref[...]

    def backward(index, carry):
        slot = items_ref[index // tiles, index % tiles]
        value = quant_ref[index]
        rows = diff_ref[index]
        by_log = rows[11:12]
        rows = rows.astype(bf16)
        colour = jnp.where((row8 >= 4) & (row8 < 7), value, jnp.where(row8 == 7, 1.0, 0.0))
        high = colour.astype(bf16).astype(f32)
        low = colour - high
        left = jnp.concatenate([high[4:8], high[4:8], low[4:8], jnp.zeros((4, BLOCK), f32)], axis=0)
        mix_ref[...] = jnp.dot(left.T.astype(bf16), rows, preferred_element_type=f32)
        for chunk in range(BLOCK // CHUNK):
            part = pl.ds(chunk * CHUNK, CHUNK)
            for half in range(2):
                pixels = pl.ds(half * BLOCK, BLOCK)
                alpha = alpha_ref[index, part, pixels]
                clear = 1.0 - alpha
                inverse = 1.0 / clear
                grad = alpha * (mix_ref[part, pixels] - by_log[:, half * BLOCK : (half + 1) * BLOCK] * inverse)
                high, low = split_pair(grad)
                lhs_ref[part, pixels] = high
                lhs_ref[part, pl.ds(PIX + half * BLOCK, BLOCK)] = low
        for block in range(2):
            lhs_ref[:, pl.ds((2 + block) * PIX, PIX)] = split_ref[index, pl.ds(block * BLOCK, BLOCK), :]
            rhs_ref[ROWS:, pl.ds((2 + block) * PIX, PIX)] = rows[0:ROWS]
        moments = lax.dot_general(lhs_ref[...], rhs_ref[...], (((1,), (1,)), ((), ())), preferred_element_type=f32).T
        inverse = value[2:3]
        base_x = 0.5 - value[0:1]
        base_y = 0.5 - value[1:2]
        zero, one_x, one_y = moments[0:1], moments[1:2] * (1.0 / SIDE), moments[2:3] * (1.0 / SIDE)
        two = (moments[3:4] + moments[4:5]) * (1.0 / (SIDE * SIDE))
        sum_x = one_x + base_x * zero
        sum_y = one_y + base_y * zero
        sum_r = two + 2.0 * (base_x * one_x + base_y * one_y) + (base_x * base_x + base_y * base_y) * zero
        by_u = 2.0 * inverse * sum_x
        by_w = 2.0 * inverse * sum_y
        back_ref[slot, 0:1, :] = xx * by_u + yx * by_w
        back_ref[slot, 1:2, :] = xy * by_u + yy * by_w
        back_ref[slot, 2:3, :] = 2.0 * inverse * sum_r
        back_ref[slot, 3:4, :] = zero * (1.0 - value[3:4] * (1.0 / opacity_cap))
        shade = value[4:7]
        back_ref[slot, 4:7, :] = (moments[8:11] + moments[12:15]) * shade * (1.0 - shade)
        return carry

    lax.fori_loop(0, count, backward, 0)


def scatter_kernel(block_ref, grads_ref, out_ref):
    capacity, owners = block_ref.shape
    out_ref[...] = jnp.zeros_like(out_ref)
    for owner in range(owners):
        for slot in range(capacity):
            block = block_ref[slot, owner]
            value = jnp.where(block >= 0, grads_ref[owner * capacity + slot], 0.0)
            out_ref[jnp.maximum(block, 0)] += value


def adam_kernel(own_ref, other_ref, params_ref, one_ref, two_ref, out_ref):
    fix_one = 1.0 - beta_one**first_step
    fix_two = 1.0 - beta_two**first_step
    components = params_ref.shape[0]
    for block in range(params_ref.shape[1] // BLOCK):
        lanes = pl.ds(block * BLOCK, BLOCK)
        grad = own_ref[block, 0:components, :]
        if other_ref is not None:
            grad = grad + other_ref[block, 0:components, :]
        one = beta_one * one_ref[:, lanes] + (1.0 - beta_one) * grad
        two = beta_two * two_ref[:, lanes] + (1.0 - beta_two) * grad * grad
        out_ref[:, lanes] = params_ref[:, lanes] - learn_rate * (one / fix_one) / (
            jnp.sqrt(two / fix_two) + adam_eps
        )


def limit(size):
    return pltpu.CompilerParams(vmem_limit_bytes=size * 1024 * 1024)


def shards(params, first_moment, second_moment, camera, slot_block, slot_anchor, tile_items, target):
    cells = lax.axis_size("cell")
    views = lax.axis_size("view")
    capacity = slot_block.shape[-1]
    tiles, depth = tile_items.shape[2:]
    channels = target.shape[3]
    per_cell = params.shape[1]
    blocks = per_cell // BLOCK
    slots = cells * capacity
    count = tiles * depth

    camera_row = camera.reshape(1, 4)
    block_ids = jnp.swapaxes(slot_block, 3, 4).reshape(capacity, cells)
    anchors = jnp.swapaxes(slot_anchor, 4, 5).reshape(2, capacity, cells)
    items = jnp.swapaxes(tile_items, 2, 3).reshape(depth, tiles)
    goals = jnp.transpose(target, (0, 1, 3, 2, 4)).reshape(channels, tiles, PIX)
    slab = jax.ShapeDtypeStruct((slots, ROWS, BLOCK), f32)

    def exchange(array):
        array = array.reshape(cells, capacity, ROWS, BLOCK)
        array = lax.all_to_all(array, "cell", split_axis=0, concat_axis=0, tiled=True)
        return array.reshape(slots, ROWS, BLOCK)

    packed = pl.pallas_call(
        pack_kernel,
        out_shape=slab,
        in_specs=[smem, smem, smem, vmem],
        out_specs=vmem,
        compiler_params=limit(4),
        name="pack",
    )(block_ids, anchors, camera_row, params)
    arrived = exchange(packed)
    back, losses = pl.pallas_call(
        owner_kernel,
        out_shape=(slab, jax.ShapeDtypeStruct((1, tiles), f32)),
        in_specs=[smem, smem, vmem, vmem, vmem, vmem],
        out_specs=(vmem, vmem),
        scratch_shapes=[
            pltpu.VMEM((count, ROWS, BLOCK), f32),
            pltpu.VMEM((4, count, BLOCK, BLOCK), f32),
            pltpu.VMEM((count, BLOCK, PIX), f32),
            pltpu.VMEM((count, 2 * BLOCK, PIX), bf16),
            pltpu.VMEM((count, ROWS, PIX), f32),
            pltpu.VMEM((count, 2 * ROWS, PIX), f32),
            pltpu.VMEM((BLOCK, PIX), f32),
            pltpu.VMEM((BLOCK, 4 * PIX), bf16),
            pltpu.VMEM((2 * ROWS, 4 * PIX), bf16),
        ],
        compiler_params=limit(40),
        name="owner",
    )(items, camera_row, arrived, goals, jnp.asarray(blur_kron()), jnp.asarray(moment_basis(), bf16))
    returned = exchange(back)
    summed = pl.pallas_call(
        scatter_kernel,
        out_shape=jax.ShapeDtypeStruct((blocks, ROWS, BLOCK), f32),
        in_specs=[smem, vmem],
        out_specs=vmem,
        compiler_params=limit(4),
        name="scatter",
    )(block_ids, returned)
    operands = [summed]
    body = adam_kernel
    if views == 2:
        operands.append(lax.ppermute(summed, "view", [(0, 1), (1, 0)]))
    else:
        operands = [lax.psum(summed, "view")]
        body = lambda own, *rest: adam_kernel(own, None, *rest)
    current = pl.pallas_call(
        body,
        out_shape=jax.ShapeDtypeStruct(params.shape, f32),
        in_specs=[vmem] * (len(operands) + 3),
        out_specs=vmem,
        compiler_params=limit(4),
        name="adam",
    )(*operands, params, first_moment, second_moment)
    return current, losses.reshape(1, 1, tiles)


def solution(mesh):
    placed = (
        P(None, "cell"),
        P(None, "cell"),
        P(None, "cell"),
        P(None, "view", None),
        P(None, "view", "cell", None, None),
        P(None, "view", "cell", None, None, None),
        P(None, "view", "cell", None),
        P(None, "view", "cell", None, None),
    )
    return jax.shard_map(
        shards,
        mesh=mesh,
        in_specs=placed,
        out_specs=(P(None, "cell"), P(None, "view", "cell")),
        check_vma=False,
    )
```

```python
import functools

import jax
import jax.numpy as jnp
import numpy as np
from jax import lax
from jax.experimental import pallas as pl
from jax.experimental.pallas import tpu as pltpu
from jax.sharding import PartitionSpec as P

SIDE = 16
BLOCK = 128
TAPS = 11
PIX = SIDE * SIDE
ROWS = 8

ssim_weight = 0.2
stable_one = 0.0001
stable_two = 0.0009
learn_rate = 0.1
beta_one = 0.9
beta_two = 0.999
adam_eps = 1e-08
first_step = 1
opacity_cap = 0.1
weight_floor = 0.5
highest = lax.Precision.HIGHEST
f32 = jnp.float32
bf16 = jnp.bfloat16
CHUNK = 16
UNROLL = (8, 8, 8, 8)

vmem = pl.BlockSpec(memory_space=pltpu.VMEM)
smem = pl.BlockSpec(memory_space=pltpu.SMEM)
hbm = pl.BlockSpec(memory_space=pltpu.HBM)


def blur_kron():
    offsets = np.arange(SIDE)[:, None] - np.arange(SIDE)[None, :]
    kernel = np.exp(-(offsets * offsets) / 4.5) * (np.abs(offsets) <= TAPS // 2)
    kernel = kernel / kernel.sum(axis=1, keepdims=True)
    return np.kron(kernel, kernel).astype(np.float32)


def pack_kernel(
    block_hbm, anchor_hbm, camera_hbm, params_hbm, items_hbm,
    out_ref, items_ref, row_ref,
    block_ref, anchor_ref, camera_ref, params_ref, sems,
):
    capacity, owners = block_ref.shape
    components = params_ref.shape[0]
    pairs = (
        (params_hbm, params_ref), (block_hbm, block_ref), (anchor_hbm, anchor_ref), (camera_hbm, camera_ref),
        (items_hbm, items_ref), (camera_hbm, row_ref),
    )
    copies = [pltpu.make_async_copy(source, target, sems.at[i]) for i, (source, target) in enumerate(pairs)]
    for copy in copies:
        copy.start()
    for copy in copies:
        copy.wait()
    xx = 1.0 + camera_ref[0, 0]
    xy = camera_ref[0, 1]
    yx = camera_ref[0, 2]
    yy = 1.0 + camera_ref[0, 3]
    for owner in range(owners):
        for slot in range(capacity):
            block = jnp.maximum(block_ref[slot, owner], 0)
            lanes = pl.ds(pl.multiple_of(block * BLOCK, BLOCK), BLOCK)
            tile = params_ref[:, lanes]
            pos_x, pos_y = tile[0:1], tile[1:2]
            row = owner * capacity + slot
            out_ref[row, 0:1, :] = xx * pos_x + xy * pos_y + anchor_ref[0, slot, owner]
            out_ref[row, 1:2, :] = yx * pos_x + yy * pos_y + anchor_ref[1, slot, owner]
            out_ref[row, 2:components, :] = tile[2:]
            out_ref[row, components:, :] = jnp.zeros((ROWS - components, BLOCK), f32)


def split_pair(value):
    high = value.astype(bf16)
    return high, (value - high.astype(f32)).astype(bf16)


def owner_kernel(
    items_ref, camera_ref, arrived_ref, goal_ref, table_ref,
    back_ref, loss_ref,
    quant_ref, left_ref, factor_ref, turned_ref, alpha_ref, split_ref, part_ref, diff_ref, lhs_ref,
):
    depth, tiles = items_ref.shape
    channels = goal_ref.shape[0]
    count = depth * tiles
    halves = PIX // BLOCK
    back_ref[...] = jnp.zeros_like(back_ref)
    row8 = lax.broadcasted_iota(jnp.int32, (ROWS, BLOCK), 0)
    places = (lax.broadcasted_iota(jnp.int32, (SIDE, BLOCK), 0).astype(f32) + 0.5) / SIDE

    def quantities(index, carry):
        slot = items_ref[index // tiles, index % tiles]
        raw = arrived_ref[slot]
        sig = jax.nn.sigmoid(raw)
        spread = 0.5 * jnp.exp(-2.0 * raw)
        value = jnp.where(row8 < 2, raw, jnp.where(row8 == 2, spread, jnp.where(row8 == 3, opacity_cap * sig, sig)))
        quant_ref[index] = value
        delta_x = places - value[0:1]
        delta_y = places - value[1:2]
        factor_x = jnp.exp(-(delta_x * delta_x) * value[2:3])
        factor_y = value[3:4] * jnp.exp(-(delta_y * delta_y) * value[2:3])
        factor_ref[index, 0:SIDE, :] = factor_x
        factor_ref[index, SIDE:, :] = factor_y
        colour = jnp.where(row8 == 7, 1.0, jnp.where(row8 >= 4, value, 0.0))
        high = colour.astype(bf16).astype(f32)
        low = colour - high
        left = jnp.concatenate([pltpu.roll(low, 5, 0), high + pltpu.roll(high, 4, 0)], axis=0)
        left_ref[index] = left.astype(bf16)
        turned_ref[index] = left.T.astype(bf16)
        return carry

    lax.fori_loop(0, count, quantities, 0, unroll=UNROLL[0])

    def forward(index, carry):
        factor_x = jnp.concatenate([factor_ref[index, 0:SIDE, :]] * (BLOCK // SIDE), axis=0).T
        factor_y = factor_ref[index, SIDE:, :]
        prods = [None] * halves
        for half in range(halves):
            tall = [
                jnp.broadcast_to(factor_y[half * ROWS + row : half * ROWS + row + 1], (SIDE, BLOCK)) for row in range(ROWS)
            ]
            tall = jnp.concatenate(tall, axis=0).T
            for chunk in range(BLOCK // CHUNK):
                rows = slice(chunk * CHUNK, (chunk + 1) * CHUNK)
                alpha = factor_x[rows] * tall[rows]
                alpha_ref[index, half, rows, :] = alpha
                high, low = split_pair(alpha)
                split_ref[index, half, rows, :] = high
                split_ref[index, half, pl.ds(BLOCK + chunk * CHUNK, CHUNK), :] = low
                clear = 1.0 - alpha
                prods[half] = clear if prods[half] is None else prods[half] * clear
        left = left_ref[index]
        right = jnp.concatenate([split_ref[index, half] for half in range(halves)], axis=1)
        sums = jnp.dot(jnp.concatenate([left, left], axis=1), right, preferred_element_type=f32)
        sums = sums[ROWS:] + pltpu.roll(sums[:ROWS], ROWS - 1, 0)
        for half in range(halves):
            prod = prods[half][:ROWS] * prods[half][ROWS:]
            for shift in (4, 2, 1):
                prod = prod * pltpu.roll(prod, shift, 0)
            part_ref[half, pl.ds(pl.multiple_of(index * ROWS, ROWS), ROWS), :] = jnp.where(
                row8 == 4, prod, sums[:, half * BLOCK : (half + 1) * BLOCK]
            )
        return carry

    lax.fori_loop(0, count, forward, 0, unroll=UNROLL[1])

    def gathered(row, rank):
        rows = pl.ds(rank * tiles * ROWS + row, tiles, stride=ROWS)
        return jnp.concatenate([part_ref[half, rows, :] for half in range(halves)], axis=1)

    transmits = [gathered(4, rank) for rank in range(depth)]
    totals = [gathered(3, rank) for rank in range(depth)]
    floors = [jnp.maximum(total, weight_floor) for total in totals]
    ratios = [(1.0 - transmit) / floor for transmit, floor in zip(transmits, floors)]
    weighted = [[gathered(ch, rank) for ch in range(channels)] for rank in range(depth)]
    shaded = [[ratios[rank] * weighted[rank][ch] for ch in range(channels)] for rank in range(depth)]
    fronts = [jnp.ones_like(transmits[0])]
    for rank in range(depth):
        fronts.append(fronts[rank] * transmits[rank])
    images = [sum(fronts[rank] * shaded[rank][ch] for rank in range(depth)) for ch in range(channels)]
    goals = [goal_ref[ch] for ch in range(channels)]
    image = jnp.concatenate(images, axis=0)
    goal = jnp.concatenate(goals, axis=0)
    stacked = jnp.concatenate([image, goal, image * image, goal * goal, image * goal], axis=0)
    blurred = lax.dot_general(stacked, table_ref[...], (((1,), (1,)), ((), ())), precision=highest, preferred_element_type=f32)
    size = channels * tiles
    local_a, local_b, square_a, square_b, cross = [blurred[i * size : (i + 1) * size] for i in range(5)]
    var_a = square_a - local_a * local_a
    var_b = square_b - local_b * local_b
    both = cross - local_a * local_b
    top_one = 2.0 * local_a * local_b + stable_one
    top_two = 2.0 * both + stable_two
    low_one = local_a * local_a + local_b * local_b + stable_one
    low_two = var_a + var_b + stable_two
    under = 1.0 / (low_one * low_two)
    similar = top_one * top_two * under
    residue = image - goal
    values = (1.0 - ssim_weight) * residue * residue + ssim_weight * (1.0 - similar)
    per_tile = values[:tiles]
    for ch in range(1, channels):
        per_tile = per_tile + values[ch * tiles : (ch + 1) * tiles]
    norm = 1.0 / (channels * PIX)
    column = jnp.sum(per_tile, axis=1, keepdims=True) * norm
    loss_ref[...] = jnp.broadcast_to(column, (tiles, BLOCK)).T[0:1, :]
    scale = -ssim_weight * norm
    by_top_one = scale * top_two * under
    by_top_two = scale * top_one * under
    by_low_one = -scale * similar / low_one
    by_low_two = -scale * similar / low_two
    by_local = 2.0 * (local_b * (by_top_one - by_top_two) + local_a * (by_low_one - by_low_two))
    spread = jnp.dot(
        jnp.concatenate([by_local, by_low_two, 2.0 * by_top_two], axis=0),
        table_ref[...], precision=highest, preferred_element_type=f32,
    )
    by_image = (
        (2.0 * (1.0 - ssim_weight) * norm) * residue
        + spread[:size] + 2.0 * image * spread[size : 2 * size] + goal * spread[2 * size :]
    )
    by_image = [by_image[ch * tiles : (ch + 1) * tiles] for ch in range(channels)]
    diff_ref[...] = jnp.zeros_like(diff_ref)

    def spread_rows(row, rank, value):
        rows = pl.ds(rank * tiles * 2 * ROWS + row, tiles, stride=2 * ROWS)
        for half in range(halves):
            diff_ref[half, rows, :] = value[:, half * BLOCK : (half + 1) * BLOCK]

    by_front = None
    for rank in reversed(range(depth)):
        by_shaded = [fronts[rank] * by_image[ch] for ch in range(channels)]
        by_transmit = -sum(by_shaded[ch] * weighted[rank][ch] for ch in range(channels)) / floors[rank]
        if by_front is not None:
            by_transmit = by_transmit + by_front * fronts[rank]
        own = sum(by_image[ch] * shaded[rank][ch] for ch in range(channels))
        by_front = own if by_front is None else own + by_front * transmits[rank]
        by_floor = -sum(by_shaded[ch] * shaded[rank][ch] for ch in range(channels)) / floors[rank]
        total = totals[rank]
        by_total = by_floor * jnp.where(total > weight_floor, 1.0, jnp.where(total == weight_floor, 0.5, 0.0))
        for q in range(4):
            value = by_shaded[q] * ratios[rank] if q < channels else by_total
            high = value.astype(bf16).astype(f32)
            spread_rows(8 + q, rank, high)
            spread_rows(12 + q, rank, value - high)
            if q < channels:
                spread_rows(1 + q, rank, high)
        spread_rows(0, rank, by_transmit * transmits[rank])

    xx = 1.0 + camera_ref[0, 0]
    xy = camera_ref[0, 1]
    yx = camera_ref[0, 2]
    yy = 1.0 + camera_ref[0, 3]

    def item_rows(index):
        rows = pl.ds(pl.multiple_of(index * 2 * ROWS, 2 * ROWS), 2 * ROWS)
        return jnp.concatenate([diff_ref[half, rows, :] for half in range(halves)], axis=1)

    def backward(index, carry):
        rows = item_rows(index)
        by_log = rows[0:1]
        mix = jnp.dot(turned_ref[index], rows.astype(bf16), preferred_element_type=f32)
        for half in range(halves):
            start = half * BLOCK
            for chunk in range(BLOCK // CHUNK):
                part = slice(chunk * CHUNK, (chunk + 1) * CHUNK)
                alpha = alpha_ref[index, half, part, :]
                inverse = 1.0 / (1.0 - alpha)
                grad = alpha * (mix[part, start : start + BLOCK] - by_log[:, start : start + BLOCK] * inverse)
                high, low = split_pair(grad)
                lhs_ref[index, half, part, :] = high
                lhs_ref[index, halves + half, part, :] = low
        return carry

    lax.fori_loop(0, count, backward, 0, unroll=UNROLL[2])

    places = lax.broadcasted_iota(jnp.int32, (2 * ROWS, PIX), 1)
    row16 = lax.broadcasted_iota(jnp.int32, (2 * ROWS, PIX), 0)
    middle = (SIDE - 1) / 2
    cell_x = (places % SIDE).astype(f32) - middle
    cell_y = (places // SIDE).astype(f32) - middle
    basis = jnp.where(row16 == 0, 1.0, 0.0)
    for row, value in enumerate((cell_x, cell_y, cell_x * cell_x, cell_y * cell_y)):
        basis = jnp.where(row16 == row + 1, value, basis)
    basis = basis.astype(bf16)
    basis = jnp.concatenate([basis, basis], axis=1)
    lower = row16 >= ROWS
    contract = (((1,), (1,)), ((), ()))

    def finish(index, carry):
        slot = items_ref[index // tiles, index % tiles]
        value = quant_ref[index]
        rows = jnp.where(lower, item_rows(index), 0.0).astype(bf16)
        left = [lhs_ref[index, i] for i in range(2 * halves)] + [split_ref[index, i, 0:BLOCK, :] for i in range(halves)]
        moments = lax.dot_general(
            jnp.concatenate(left, axis=1), jnp.concatenate([basis, rows], axis=1), contract, preferred_element_type=f32
        )
        moments = moments.T
        inverse = value[2:3]
        base_x = 0.5 - value[0:1]
        base_y = 0.5 - value[1:2]
        zero, one_x, one_y = moments[0:1], moments[1:2] * (1.0 / SIDE), moments[2:3] * (1.0 / SIDE)
        two = (moments[3:4] + moments[4:5]) * (1.0 / (SIDE * SIDE))
        sum_x = one_x + base_x * zero
        sum_y = one_y + base_y * zero
        sum_r = two + 2.0 * (base_x * one_x + base_y * one_y) + (base_x * base_x + base_y * base_y) * zero
        by_u = 2.0 * inverse * sum_x
        by_w = 2.0 * inverse * sum_y
        back_ref[slot, 0:1, :] = xx * by_u + yx * by_w
        back_ref[slot, 1:2, :] = xy * by_u + yy * by_w
        back_ref[slot, 2:3, :] = 2.0 * inverse * sum_r
        back_ref[slot, 3:4, :] = zero * (1.0 - value[3:4] * (1.0 / opacity_cap))
        shade = value[4:7]
        back_ref[slot, 4:7, :] = (moments[8:11] + moments[12:15]) * shade * (1.0 - shade)
        return carry

    lax.fori_loop(0, count, finish, 0, unroll=UNROLL[3])


def scatter_kernel(block_ref, grads_ref, out_ref, *spare_refs):
    capacity, owners = block_ref.shape
    sums = (out_ref, *spare_refs)
    for target in sums:
        target[...] = jnp.zeros_like(target)
    for index in range(owners * capacity):
        block = block_ref[index % capacity, index // capacity]
        value = jnp.where(block >= 0, grads_ref[index], 0.0)
        sums[index % len(sums)][jnp.maximum(block, 0)] += value
    out_ref[...] = sum(target[...] for target in sums)


def adam_kernel(own_ref, other_ref, params_ref, one_ref, two_ref, out_ref):
    fix_one = 1.0 - beta_one**first_step
    fix_two = 1.0 - beta_two**first_step
    components = params_ref.shape[0]
    for block in range(params_ref.shape[1] // BLOCK):
        lanes = pl.ds(block * BLOCK, BLOCK)
        grad = own_ref[block, 0:components, :]
        if other_ref is not None:
            grad = grad + other_ref[block, 0:components, :]
        one = beta_one * one_ref[:, lanes] + (1.0 - beta_one) * grad
        two = beta_two * two_ref[:, lanes] + (1.0 - beta_two) * grad * grad
        out_ref[:, lanes] = params_ref[:, lanes] - learn_rate * (one / fix_one) / (
            jnp.sqrt(two / fix_two) + adam_eps
        )


def limit(size):
    return pltpu.CompilerParams(vmem_limit_bytes=size * 1024 * 1024)


def shards(params, first_moment, second_moment, camera, slot_block, slot_anchor, tile_items, target):
    cells = lax.axis_size("cell")
    views = lax.axis_size("view")
    capacity = slot_block.shape[-1]
    tiles, depth = tile_items.shape[2:]
    channels = target.shape[3]
    per_cell = params.shape[1]
    blocks = per_cell // BLOCK
    slots = cells * capacity
    count = tiles * depth
    halves = PIX // BLOCK

    camera_row = camera.reshape(1, 4)
    block_ids = jnp.swapaxes(slot_block, 3, 4).reshape(capacity, cells)
    anchors = jnp.swapaxes(slot_anchor, 4, 5).reshape(2, capacity, cells)
    items = jnp.swapaxes(tile_items, 2, 3).reshape(depth, tiles)
    goals = jnp.transpose(target, (0, 1, 3, 2, 4)).reshape(channels, tiles, PIX)
    slab = jax.ShapeDtypeStruct((slots, ROWS, BLOCK), f32)

    def exchange(array):
        array = array.reshape(cells, capacity, ROWS, BLOCK)
        array = lax.all_to_all(array, "cell", split_axis=0, concat_axis=0, tiled=True)
        return array.reshape(slots, ROWS, BLOCK)

    packed, items, camera_row = pl.pallas_call(
        pack_kernel,
        out_shape=(slab, jax.ShapeDtypeStruct(items.shape, items.dtype), jax.ShapeDtypeStruct(camera_row.shape, f32)),
        in_specs=[hbm] * 5,
        out_specs=(vmem, vmem, vmem),
        scratch_shapes=[
            pltpu.SMEM(block_ids.shape, jnp.int32),
            pltpu.SMEM(anchors.shape, f32),
            pltpu.SMEM(camera_row.shape, f32),
            pltpu.VMEM(params.shape, f32),
            pltpu.SemaphoreType.DMA((6,)),
        ],
        compiler_params=limit(4),
        name="pack",
    )(*[pltpu.with_memory_space_constraint(array, pltpu.HBM) for array in (block_ids, anchors, camera_row, params, items)])
    arrived = exchange(packed)
    back, losses = pl.pallas_call(
        owner_kernel,
        out_shape=(slab, jax.ShapeDtypeStruct((1, tiles), f32)),
        in_specs=[smem, smem, vmem, vmem, vmem],
        out_specs=(vmem, vmem),
        scratch_shapes=[
            pltpu.VMEM((count, ROWS, BLOCK), f32),
            pltpu.VMEM((count, 2 * ROWS, BLOCK), bf16),
            pltpu.VMEM((count, 2 * SIDE, BLOCK), f32),
            pltpu.VMEM((count, BLOCK, 2 * ROWS), bf16),
            pltpu.VMEM((count, halves, BLOCK, BLOCK), f32),
            pltpu.VMEM((count, halves, 2 * BLOCK, BLOCK), bf16),
            pltpu.VMEM((halves, count * ROWS, BLOCK), f32),
            pltpu.VMEM((halves, count * 2 * ROWS, BLOCK), f32),
            pltpu.VMEM((count, 2 * halves, BLOCK, BLOCK), bf16),
        ],
        compiler_params=limit(40),
        name="owner",
    )(items, camera_row, arrived, goals, jnp.asarray(blur_kron()))
    returned = exchange(back)
    summed = pl.pallas_call(
        scatter_kernel,
        out_shape=jax.ShapeDtypeStruct((blocks, ROWS, BLOCK), f32),
        in_specs=[smem, vmem],
        out_specs=vmem,
        scratch_shapes=[pltpu.VMEM((blocks, ROWS, BLOCK), f32)] * 3,
        compiler_params=limit(4),
        name="scatter",
    )(block_ids, returned)
    operands = [summed]
    body = adam_kernel
    if views == 2:
        operands.append(lax.ppermute(summed, "view", [(0, 1), (1, 0)]))
    else:
        operands = [lax.psum(summed, "view")]
        body = lambda own, *rest: adam_kernel(own, None, *rest)
    current = pl.pallas_call(
        body,
        out_shape=jax.ShapeDtypeStruct(params.shape, f32),
        in_specs=[vmem] * (len(operands) + 3),
        out_specs=vmem,
        compiler_params=limit(4),
        name="adam",
    )(*operands, params, first_moment, second_moment)
    return current, losses.reshape(1, 1, tiles)


def solution(mesh):
    placed = (
        P(None, "cell"),
        P(None, "cell"),
        P(None, "cell"),
        P(None, "view", None),
        P(None, "view", "cell", None, None),
        P(None, "view", "cell", None, None, None),
        P(None, "view", "cell", None),
        P(None, "view", "cell", None, None),
    )
    return jax.shard_map(
        shards,
        mesh=mesh,
        in_specs=placed,
        out_specs=(P(None, "cell"), P(None, "view", "cell")),
        check_vma=False,
    )
```

```python
import functools

import jax
import jax.numpy as jnp
import numpy as np
from jax import lax
from jax.experimental import pallas as pl
from jax.experimental.pallas import tpu as pltpu
from jax.sharding import PartitionSpec as P

SIDE = 16
BLOCK = 128
TAPS = 11
PIX = SIDE * SIDE
ROWS = 8
PARAMS = 7

ssim_weight = 0.2
stable_one = 0.0001
stable_two = 0.0009
learn_rate = 0.1
beta_one = 0.9
beta_two = 0.999
adam_eps = 1e-08
first_step = 1
opacity_cap = 0.1
weight_floor = 0.5
f32 = jnp.float32
bf16 = jnp.bfloat16
CHUNK = 16
UNROLL = 32

vmem = pl.BlockSpec(memory_space=pltpu.VMEM)
hbm = pl.BlockSpec(memory_space=pltpu.HBM)


def blur_kron():
    offsets = np.arange(SIDE)[:, None] - np.arange(SIDE)[None, :]
    kernel = np.exp(-(offsets * offsets) / 4.5) * (np.abs(offsets) <= TAPS // 2)
    kernel = kernel / kernel.sum(axis=1, keepdims=True)
    table, parts = np.kron(kernel, kernel).astype(np.float32), []
    for _ in range(3):
        parts.append(table.astype(bf16))
        table = table - parts[-1].astype(np.float32)
    return np.stack(parts)


def pack_kernel(
    block_hbm, anchor_hbm, camera_hbm, params_hbm, items_hbm,
    out_ref, items_ref, row_ref, ids_ref,
    block_ref, anchor_ref, camera_ref, params_ref, sems,
):
    capacity, owners = block_ref.shape
    components = params_ref.shape[0]
    pairs = (
        (params_hbm, params_ref), (block_hbm, block_ref), (anchor_hbm, anchor_ref), (camera_hbm, camera_ref),
        (items_hbm, items_ref), (camera_hbm, row_ref),
    )
    copies = [pltpu.make_async_copy(source, target, sems.at[i]) for i, (source, target) in enumerate(pairs)]
    for copy in copies:
        copy.start()
    for copy in copies:
        copy.wait()
    xx = 1.0 + camera_ref[0, 0]
    xy = camera_ref[0, 1]
    yx = camera_ref[0, 2]
    yy = 1.0 + camera_ref[0, 3]
    slots = owners * capacity
    lane = lax.broadcasted_iota(jnp.int32, ids_ref.shape, 1)
    lane = jnp.where(lane < 3 * slots, lane % slots, -1)
    ids = jnp.full(ids_ref.shape, -1, jnp.int32)
    for index in range(slots):
        owner, slot = index // capacity, index % capacity
        block = block_ref[slot, owner]
        ids = jnp.where(lane == index, block, ids)
        lanes = pl.ds(pl.multiple_of(jnp.maximum(block, 0) * BLOCK, BLOCK), BLOCK)
        tile = params_ref[:, lanes]
        pos_x, pos_y = tile[0:1], tile[1:2]
        row = index * components
        out_ref[row : row + 1, :] = xx * pos_x + xy * pos_y + anchor_ref[0, slot, owner]
        out_ref[row + 1 : row + 2, :] = yx * pos_x + yy * pos_y + anchor_ref[1, slot, owner]
        out_ref[row + 2 : row + components, :] = tile[2:]
    ids_ref[...] = ids


def split_pair(value):
    high = value.astype(bf16)
    return high, (value - high.astype(f32)).astype(bf16)


def precise_dot(value, table_ref, dims):
    rows = value.shape[0]
    parts, rest = [], value
    for _ in range(3):
        parts.append(rest.astype(bf16))
        rest = rest - parts[-1].astype(f32)
    total = None
    for index in range(3):
        left = jnp.concatenate(parts[: 3 - index], axis=0)
        product = lax.dot_general(left, table_ref[index], (dims, ((), ())), preferred_element_type=f32)
        for part in range(3 - index):
            piece = product[part * rows : (part + 1) * rows]
            total = piece if total is None else total + piece
    return total


def padded_rows(values):
    rows = sum(value.shape[0] for value in values)
    extra = -rows % (2 * ROWS)
    if extra:
        values = values + [jnp.zeros((extra, values[0].shape[1]), f32)]
    return jnp.concatenate(values, axis=0)


def owner_kernel(
    items_vmem, camera_vmem, packed_ref, goal_ref, table_ref,
    packed_back_ref, loss_ref,
    items_ref, camera_ref, sems, arrived_ref, back_ref, quant_ref, left_ref, alpha_ref, split_ref, part_ref, diff_ref, mix_ref, grad_ref,
):
    depth, tiles = items_ref.shape
    channels = goal_ref.shape[0]
    count = depth * tiles
    halves = PIX // BLOCK
    slots = arrived_ref.shape[0]
    components = packed_ref.shape[0] // slots
    copies = [
        pltpu.make_async_copy(items_vmem, items_ref, sems.at[0]),
        pltpu.make_async_copy(camera_vmem, camera_ref, sems.at[1]),
    ]
    for copy in copies:
        copy.start()
    back_ref[...] = jnp.zeros_like(back_ref)
    for slot in range(slots):
        kept = min(ROWS, packed_ref.shape[0] - slot * components)
        arrived_ref[slot, 0:kept, :] = packed_ref[slot * components : slot * components + kept, :]
        if kept < ROWS:
            arrived_ref[slot, kept:, :] = jnp.zeros((ROWS - kept, BLOCK), f32)
    goal = jnp.concatenate([goal_ref[ch] for ch in range(channels)], axis=0)
    size = channels * tiles
    blurred_goal = precise_dot(padded_rows([goal, goal * goal]), table_ref, ((1,), (1,)))
    local_b, square_b = blurred_goal[:size], blurred_goal[size : 2 * size]
    for copy in copies:
        copy.wait()
    row8 = lax.broadcasted_iota(jnp.int32, (ROWS, BLOCK), 0)
    places = (lax.broadcasted_iota(jnp.int32, (SIDE, BLOCK), 0).astype(f32) + 0.5) / SIDE

    def forward(index, carry):
        slot = items_ref[index // tiles, index % tiles]
        raw = arrived_ref[slot]
        sig = jax.nn.sigmoid(raw)
        spread = 0.5 * jnp.exp(-2.0 * raw)
        value = jnp.where(row8 < 2, raw, jnp.where(row8 == 2, spread, jnp.where(row8 == 3, opacity_cap * sig, sig)))
        quant_ref[index] = value
        delta_x = places - value[0:1]
        delta_y = places - value[1:2]
        factor_x = jnp.exp(-(delta_x * delta_x) * value[2:3])
        factor_y = value[3:4] * jnp.exp(-(delta_y * delta_y) * value[2:3])
        colour = jnp.where(row8 == 7, 1.0, jnp.where(row8 >= 4, value, 0.0))
        high = colour.astype(bf16).astype(f32)
        low = colour - high
        left = jnp.concatenate([pltpu.roll(low, 5, 0), high + pltpu.roll(high, 4, 0)], axis=0)
        left_ref[index] = left
        left = left.astype(bf16)
        factor_x = jnp.concatenate([factor_x] * (BLOCK // SIDE), axis=0).T
        prods, rights = [], []
        for half in range(halves):
            tall = [
                jnp.broadcast_to(factor_y[half * ROWS + row : half * ROWS + row + 1], (SIDE, BLOCK)) for row in range(ROWS)
            ]
            tall = jnp.concatenate(tall, axis=0).T
            prod, highs, lows = None, [], []
            for chunk in range(BLOCK // CHUNK):
                rows = slice(chunk * CHUNK, (chunk + 1) * CHUNK)
                alpha = factor_x[rows] * tall[rows]
                alpha_ref[index, half, rows, :] = alpha
                high, low = split_pair(alpha)
                split_ref[half, pl.ds(pl.multiple_of(index * BLOCK + chunk * CHUNK, CHUNK), CHUNK), :] = high
                highs.append(high)
                lows.append(low)
                clear = 1.0 - alpha
                prod = clear if prod is None else prod * clear
            prods.append(prod)
            rights.append(jnp.concatenate(highs + lows, axis=0))
        sums = jnp.dot(
            jnp.concatenate([left, left], axis=1), jnp.concatenate(rights, axis=1), preferred_element_type=f32
        )
        sums = sums[ROWS:] + pltpu.roll(sums[:ROWS], ROWS - 1, 0)
        for half in range(halves):
            prod = prods[half][:ROWS] * prods[half][ROWS:]
            for shift in (4, 2, 1):
                prod = prod * pltpu.roll(prod, shift, 0)
            part_ref[half, pl.ds(pl.multiple_of(index * ROWS, ROWS), ROWS), :] = jnp.where(
                row8 == 4, prod, sums[:, half * BLOCK : (half + 1) * BLOCK]
            )
        return carry

    lax.fori_loop(0, count, forward, 0, unroll=UNROLL)

    def gathered(row, rank):
        rows = pl.ds(rank * tiles * ROWS + row, tiles, stride=ROWS)
        return jnp.concatenate([part_ref[half, rows, :] for half in range(halves)], axis=1)

    transmits = [gathered(4, rank) for rank in range(depth)]
    totals = [gathered(3, rank) for rank in range(depth)]
    floors = [jnp.maximum(total, weight_floor) for total in totals]
    ratios = [(1.0 - transmit) / floor for transmit, floor in zip(transmits, floors)]
    weighted = [[gathered(ch, rank) for ch in range(channels)] for rank in range(depth)]
    shaded = [[ratios[rank] * weighted[rank][ch] for ch in range(channels)] for rank in range(depth)]
    fronts = [jnp.ones_like(transmits[0])]
    for rank in range(depth):
        fronts.append(fronts[rank] * transmits[rank])
    images = [sum(fronts[rank] * shaded[rank][ch] for rank in range(depth)) for ch in range(channels)]
    image = jnp.concatenate(images, axis=0)
    blurred = precise_dot(padded_rows([image, image * image, image * goal]), table_ref, ((1,), (1,)))
    local_a, square_a, cross = [blurred[i * size : (i + 1) * size] for i in range(3)]
    var_a = square_a - local_a * local_a
    var_b = square_b - local_b * local_b
    both = cross - local_a * local_b
    top_one = 2.0 * local_a * local_b + stable_one
    top_two = 2.0 * both + stable_two
    low_one = local_a * local_a + local_b * local_b + stable_one
    low_two = var_a + var_b + stable_two
    under = 1.0 / (low_one * low_two)
    similar = top_one * top_two * under
    residue = image - goal
    values = (1.0 - ssim_weight) * residue * residue + ssim_weight * (1.0 - similar)
    per_tile = values[:tiles]
    for ch in range(1, channels):
        per_tile = per_tile + values[ch * tiles : (ch + 1) * tiles]
    norm = 1.0 / (channels * PIX)
    column = jnp.sum(per_tile, axis=1, keepdims=True) * norm
    loss_ref[...] = jnp.broadcast_to(column, (tiles, BLOCK)).T[0:1, :]
    scale = -ssim_weight * norm
    by_top_one = scale * top_two * under
    by_top_two = scale * top_one * under
    by_low_one = -scale * similar / low_one
    by_low_two = -scale * similar / low_two
    by_local = 2.0 * (local_b * (by_top_one - by_top_two) + local_a * (by_low_one - by_low_two))
    spread = precise_dot(padded_rows([by_local, by_low_two, 2.0 * by_top_two]), table_ref, ((1,), (0,)))
    by_image = (
        (2.0 * (1.0 - ssim_weight) * norm) * residue
        + spread[:size] + 2.0 * image * spread[size : 2 * size] + goal * spread[2 * size : 3 * size]
    )
    by_image = [by_image[ch * tiles : (ch + 1) * tiles] for ch in range(channels)]
    diff_ref[...] = jnp.zeros_like(diff_ref)

    def spread_rows(row, rank, value):
        rows = pl.ds(rank * tiles * 2 * ROWS + row, tiles, stride=2 * ROWS)
        for half in range(halves):
            diff_ref[half, rows, :] = value[:, half * BLOCK : (half + 1) * BLOCK]

    by_front = None
    for rank in reversed(range(depth)):
        by_shaded = [fronts[rank] * by_image[ch] for ch in range(channels)]
        by_transmit = -sum(by_shaded[ch] * weighted[rank][ch] for ch in range(channels)) / floors[rank]
        if by_front is not None:
            by_transmit = by_transmit + by_front * fronts[rank]
        own = sum(by_image[ch] * shaded[rank][ch] for ch in range(channels))
        by_front = own if by_front is None else own + by_front * transmits[rank]
        by_floor = -sum(by_shaded[ch] * shaded[rank][ch] for ch in range(channels)) / floors[rank]
        total = totals[rank]
        by_total = by_floor * jnp.where(total > weight_floor, 1.0, jnp.where(total == weight_floor, 0.5, 0.0))
        for q in range(4):
            value = by_shaded[q] * ratios[rank] if q < channels else by_total
            high = value.astype(bf16).astype(f32)
            spread_rows(8 + q, rank, high)
            spread_rows(12 + q, rank, value - high)
            if q < channels:
                spread_rows(1 + q, rank, high)
        spread_rows(0, rank, by_transmit * transmits[rank])

    xx = 1.0 + camera_ref[0, 0]
    xy = camera_ref[0, 1]
    yx = camera_ref[0, 2]
    yy = 1.0 + camera_ref[0, 3]

    group = BLOCK // (2 * ROWS)
    span = group * BLOCK
    places = lax.broadcasted_iota(jnp.int32, (BLOCK, PIX), 1)
    column = lax.broadcasted_iota(jnp.int32, (BLOCK, PIX), 0)
    middle = (SIDE - 1) / 2
    cell_x = (places % SIDE).astype(f32) - middle
    cell_y = (places // SIDE).astype(f32) - middle
    basis = jnp.where(column == ROWS // 2, 1.0, 0.0)
    for free, value in zip((5, 6, 7, 20), (cell_x, cell_y, cell_x * cell_x, cell_y * cell_y)):
        basis = jnp.where(column == free, value, basis)
    basis = basis.astype(bf16)
    basis = jnp.concatenate([basis, basis], axis=1)
    contract = (((1,), (1,)), ((), ()))

    def backward(step):
        block = pl.ds(step * BLOCK, BLOCK)
        wide = pl.ds(step * span, span)
        rows = jnp.concatenate([diff_ref[half, block, :] for half in range(halves)], axis=1).astype(bf16)
        turned = []
        for item in range(group):
            pieces = [left_ref[step * group + item]]
            if item:
                pieces.insert(0, jnp.zeros((item * 2 * ROWS, BLOCK), f32))
            if item < group - 1:
                pieces.append(jnp.zeros(((group - 1 - item) * 2 * ROWS, BLOCK), f32))
            turned.append(jnp.concatenate(pieces, axis=0).T.astype(bf16))
        mix = jnp.dot(jnp.concatenate(turned, axis=0), rows, preferred_element_type=f32)
        for half in range(halves):
            mix_ref[step, half] = mix[:, half * BLOCK : (half + 1) * BLOCK]
        for item in range(group):
            index = step * group + item
            for half in range(halves):
                by_log = diff_ref[half, pl.ds(index * 2 * ROWS, 1), :]
                for chunk in range(BLOCK // CHUNK):
                    alpha = alpha_ref[index, half, chunk * CHUNK : (chunk + 1) * CHUNK, :]
                    inverse = 1.0 / (1.0 - alpha)
                    first = item * BLOCK + chunk * CHUNK
                    grad = alpha * (mix_ref[step, half, first : first + CHUNK, :] - by_log * inverse)
                    high, low = split_pair(grad)
                    grad_ref[step, half, first : first + CHUNK, :] = high
                    grad_ref[step, halves + half, first : first + CHUNK, :] = low
        left = [grad_ref[step, i] for i in range(2 * halves)] + [split_ref[half, wide, :] for half in range(halves)]
        totals = lax.dot_general(
            jnp.concatenate(left, axis=1), jnp.concatenate([basis, rows], axis=1), contract, preferred_element_type=f32
        )
        for item in range(group):
            finish(step * group + item, item, totals[item * BLOCK : (item + 1) * BLOCK].T)

    def finish(index, item, moments):
        slot = items_ref[index // tiles, index % tiles]
        value = quant_ref[index]
        inverse = value[2:3]
        base_x = 0.5 - value[0:1]
        base_y = 0.5 - value[1:2]
        zero, one_x, one_y = moments[4:5], moments[5:6] * (1.0 / SIDE), moments[6:7] * (1.0 / SIDE)
        two = (moments[7:8] + moments[20:21]) * (1.0 / (SIDE * SIDE))
        sum_x = one_x + base_x * zero
        sum_y = one_y + base_y * zero
        sum_r = two + 2.0 * (base_x * one_x + base_y * one_y) + (base_x * base_x + base_y * base_y) * zero
        by_u = 2.0 * inverse * sum_x
        by_w = 2.0 * inverse * sum_y
        back_ref[slot, 0:1, :] = xx * by_u + yx * by_w
        back_ref[slot, 1:2, :] = xy * by_u + yy * by_w
        back_ref[slot, 2:3, :] = 2.0 * inverse * sum_r
        back_ref[slot, 3:4, :] = zero * (1.0 - value[3:4] * (1.0 / opacity_cap))
        shade = value[4:7]
        first = item * 2 * ROWS + ROWS
        back_ref[slot, 4:7, :] = (moments[first : first + 3] + moments[first + 4 : first + 7]) * shade * (1.0 - shade)

    for step in range(count // group):
        backward(step)
    for slot in range(slots):
        packed_back_ref[slot * components : (slot + 1) * components, :] = back_ref[slot, 0:components, :]


def scatter_kernel(ids_ref, grads_ref, out_ref):
    lanes = ids_ref.shape[1]
    components = PARAMS
    slots = grads_ref.shape[0] // components
    blocks = out_ref.shape[0] // components
    block = lax.broadcasted_iota(jnp.int32, (blocks, lanes), 0)
    chosen = jnp.where(block == ids_ref[0:1, :], 1.0, 0.0).astype(bf16)
    columns = []
    for row in range(components):
        rest, parts = grads_ref[pl.ds(row, slots, stride=components), :], []
        for _ in range(3):
            parts.append(rest.astype(bf16))
            rest = rest - parts[-1].astype(f32)
        if lanes > 3 * slots:
            parts.append(jnp.zeros((lanes - 3 * slots, BLOCK), bf16))
        columns.append(jnp.concatenate(parts, axis=0))
    sums = jnp.dot(chosen, jnp.concatenate(columns, axis=1), preferred_element_type=f32)
    for row in range(components):
        out_ref[pl.ds(row, blocks, stride=components), :] = sums[:, row * BLOCK : (row + 1) * BLOCK]


def adam_kernel(own_ref, other_ref, params_ref, one_ref, two_ref, out_ref):
    fix_one = 1.0 - beta_one**first_step
    fix_two = 1.0 - beta_two**first_step
    components = params_ref.shape[0]
    for block in range(params_ref.shape[1] // BLOCK):
        lanes = pl.ds(block * BLOCK, BLOCK)
        rows = slice(block * components, (block + 1) * components)
        grad = own_ref[rows, :]
        if other_ref is not None:
            grad = grad + other_ref[rows, :]
        one = beta_one * one_ref[:, lanes] + (1.0 - beta_one) * grad
        two = beta_two * two_ref[:, lanes] + (1.0 - beta_two) * grad * grad
        out_ref[:, lanes] = params_ref[:, lanes] - learn_rate * (one / fix_one) / (
            jnp.sqrt(two / fix_two) + adam_eps
        )


def limit(size):
    return pltpu.CompilerParams(vmem_limit_bytes=size * 1024 * 1024)


def shards(params, first_moment, second_moment, camera, slot_block, slot_anchor, tile_items, target):
    cells = lax.axis_size("cell")
    views = lax.axis_size("view")
    capacity = slot_block.shape[-1]
    tiles, depth = tile_items.shape[2:]
    channels = target.shape[3]
    per_cell = params.shape[1]
    blocks = per_cell // BLOCK
    slots = cells * capacity
    count = tiles * depth
    halves = PIX // BLOCK
    span = BLOCK // (2 * ROWS) * BLOCK

    camera_row = camera.reshape(1, 4)
    block_ids = jnp.swapaxes(slot_block, 3, 4).reshape(capacity, cells)
    anchors = jnp.swapaxes(slot_anchor, 4, 5).reshape(2, capacity, cells)
    items = jnp.swapaxes(tile_items, 2, 3).reshape(depth, tiles)
    goals = jnp.transpose(target, (0, 1, 3, 2, 4)).reshape(channels, tiles, PIX)
    slab = jax.ShapeDtypeStruct((slots * PARAMS, BLOCK), f32)
    id_lanes = -(-3 * slots // BLOCK) * BLOCK

    def exchange(array):
        array = array.reshape(cells, 1, capacity * PARAMS * BLOCK)
        array = lax.all_to_all(array, "cell", split_axis=0, concat_axis=0, tiled=True)
        return array.reshape(slots * PARAMS, BLOCK)

    packed, items, camera_row, ids = pl.pallas_call(
        pack_kernel,
        out_shape=(slab, jax.ShapeDtypeStruct(items.shape, items.dtype), jax.ShapeDtypeStruct(camera_row.shape, f32),
                   jax.ShapeDtypeStruct((ROWS, id_lanes), jnp.int32)),
        in_specs=[hbm] * 5,
        out_specs=(vmem,) * 4,
        scratch_shapes=[
            pltpu.SMEM(block_ids.shape, jnp.int32),
            pltpu.SMEM(anchors.shape, f32),
            pltpu.SMEM(camera_row.shape, f32),
            pltpu.VMEM(params.shape, f32),
            pltpu.SemaphoreType.DMA((6,)),
        ],
        compiler_params=limit(4),
        name="pack",
    )(*[pltpu.with_memory_space_constraint(array, pltpu.HBM) for array in (block_ids, anchors, camera_row, params, items)])
    arrived = exchange(packed)
    back, losses = pl.pallas_call(
        owner_kernel,
        out_shape=(slab, jax.ShapeDtypeStruct((1, tiles), f32)),
        in_specs=[vmem] * 5,
        out_specs=(vmem, vmem),
        scratch_shapes=[
            pltpu.SMEM(items.shape, jnp.int32),
            pltpu.SMEM(camera_row.shape, f32),
            pltpu.SemaphoreType.DMA((2,)),
            pltpu.VMEM((slots, ROWS, BLOCK), f32),
            pltpu.VMEM((slots, ROWS, BLOCK), f32),
            pltpu.VMEM((count, ROWS, BLOCK), f32),
            pltpu.VMEM((count, 2 * ROWS, BLOCK), f32),
            pltpu.VMEM((count, halves, BLOCK, BLOCK), f32),
            pltpu.VMEM((halves, count * BLOCK, BLOCK), bf16),
            pltpu.VMEM((halves, count * ROWS, BLOCK), f32),
            pltpu.VMEM((halves, count * 2 * ROWS, BLOCK), f32),
            pltpu.VMEM((count * BLOCK // span, halves, span, BLOCK), f32),
            pltpu.VMEM((count * BLOCK // span, 2 * halves, span, BLOCK), bf16),
        ],
        compiler_params=limit(40),
        name="owner",
    )(items, camera_row, arrived, goals, jnp.asarray(blur_kron()))
    returned = exchange(back)
    summed = pl.pallas_call(
        scatter_kernel,
        out_shape=jax.ShapeDtypeStruct((blocks * PARAMS, BLOCK), f32),
        in_specs=[vmem, vmem],
        out_specs=vmem,
        compiler_params=limit(4),
        name="scatter",
    )(ids, returned)
    operands = [summed]
    body = adam_kernel
    if views == 2:
        operands.append(lax.ppermute(summed, "view", [(0, 1), (1, 0)]))
    else:
        operands = [lax.psum(summed, "view")]
        body = lambda own, *rest: adam_kernel(own, None, *rest)
    current = pl.pallas_call(
        body,
        out_shape=jax.ShapeDtypeStruct(params.shape, f32),
        in_specs=[vmem] * (len(operands) + 3),
        out_specs=vmem,
        compiler_params=limit(4),
        name="adam",
    )(*operands, params, first_moment, second_moment)
    return current, losses.reshape(1, 1, tiles)


def solution(mesh):
    placed = (
        P(None, "cell"),
        P(None, "cell"),
        P(None, "cell"),
        P(None, "view", None),
        P(None, "view", "cell", None, None),
        P(None, "view", "cell", None, None, None),
        P(None, "view", "cell", None),
        P(None, "view", "cell", None, None),
    )
    return jax.shard_map(
        shards,
        mesh=mesh,
        in_specs=placed,
        out_specs=(P(None, "cell"), P(None, "view", "cell")),
        check_vma=False,
    )
```

```python
import functools

import jax
import jax.numpy as jnp
import numpy as np
from jax import lax
from jax.experimental import pallas as pl
from jax.experimental.pallas import tpu as pltpu
from jax.sharding import PartitionSpec as P

SIDE = 16
BLOCK = 128
TAPS = 11
PIX = SIDE * SIDE
ROWS = 8
PARAMS = 7

ssim_weight = 0.2
stable_one = 0.0001
stable_two = 0.0009
learn_rate = 0.1
beta_one = 0.9
beta_two = 0.999
adam_eps = 1e-08
first_step = 1
opacity_cap = 0.1
weight_floor = 0.5
f32 = jnp.float32
bf16 = jnp.bfloat16
CHUNK = 16
UNROLL = 32

vmem = pl.BlockSpec(memory_space=pltpu.VMEM)
hbm = pl.BlockSpec(memory_space=pltpu.HBM)


def blur_kron():
    offsets = np.arange(SIDE)[:, None] - np.arange(SIDE)[None, :]
    kernel = np.exp(-(offsets * offsets) / 4.5) * (np.abs(offsets) <= TAPS // 2)
    kernel = kernel / kernel.sum(axis=1, keepdims=True)
    table, parts = np.kron(kernel, kernel).astype(np.float32), []
    for _ in range(3):
        parts.append(table.astype(bf16))
        table = table - parts[-1].astype(np.float32)
    return np.stack(parts)


def pack_kernel(
    block_hbm, anchor_hbm, camera_hbm, params_hbm, items_hbm,
    out_ref, items_ref, row_ref, ids_ref,
    block_ref, anchor_ref, camera_ref, params_ref, sems,
):
    capacity, owners = block_ref.shape
    components = params_ref.shape[0]
    pairs = (
        (params_hbm, params_ref), (block_hbm, block_ref), (anchor_hbm, anchor_ref), (camera_hbm, camera_ref),
        (items_hbm, items_ref), (camera_hbm, row_ref),
    )
    copies = [pltpu.make_async_copy(source, target, sems.at[i]) for i, (source, target) in enumerate(pairs)]
    for copy in copies:
        copy.start()
    for copy in copies[1:]:
        copy.wait()
    xx = 1.0 + camera_ref[0, 0]
    xy = camera_ref[0, 1]
    yx = camera_ref[0, 2]
    yy = 1.0 + camera_ref[0, 3]
    slots = owners * capacity
    lane = lax.broadcasted_iota(jnp.int32, ids_ref.shape, 1)
    lane = jnp.where(lane < 3 * slots, lane % slots, -1)
    ids = jnp.full(ids_ref.shape, -1, jnp.int32)
    for index in range(slots):
        ids = jnp.where(lane == index, block_ref[index % capacity, index // capacity], ids)
    ids_ref[...] = ids
    copies[0].wait()
    for index in range(slots):
        owner, slot = index // capacity, index % capacity
        block = block_ref[slot, owner]
        lanes = pl.ds(pl.multiple_of(jnp.maximum(block, 0) * BLOCK, BLOCK), BLOCK)
        tile = params_ref[:, lanes]
        pos_x, pos_y = tile[0:1], tile[1:2]
        row = index * components
        out_ref[row : row + 1, :] = xx * pos_x + xy * pos_y + anchor_ref[0, slot, owner]
        out_ref[row + 1 : row + 2, :] = yx * pos_x + yy * pos_y + anchor_ref[1, slot, owner]
        out_ref[row + 2 : row + components, :] = tile[2:]


def split_pair(value):
    high = value.astype(bf16)
    return high, (value - high.astype(f32)).astype(bf16)


def precise_dot(value, table_ref, dims):
    rows = value.shape[0]
    parts, rest = [], value
    for _ in range(3):
        parts.append(rest.astype(bf16))
        rest = rest - parts[-1].astype(f32)
    total = None
    for index in range(3):
        left = jnp.concatenate(parts[: 3 - index], axis=0)
        product = lax.dot_general(left, table_ref[index], (dims, ((), ())), preferred_element_type=f32)
        for part in range(3 - index):
            piece = product[part * rows : (part + 1) * rows]
            total = piece if total is None else total + piece
    return total


def padded_rows(values):
    rows = sum(value.shape[0] for value in values)
    extra = -rows % (2 * ROWS)
    if extra:
        values = values + [jnp.zeros((extra, values[0].shape[1]), f32)]
    return jnp.concatenate(values, axis=0)


def owner_kernel(
    items_vmem, camera_vmem, packed_ref, goal_ref, table_ref,
    packed_back_ref, loss_hbm,
    items_ref, camera_ref, loss_ref, sems, arrived_ref, back_ref, quant_ref, left_ref, alpha_ref, split_ref, part_ref, diff_ref,
):
    depth, tiles = items_ref.shape
    channels = goal_ref.shape[0]
    count = depth * tiles
    halves = PIX // BLOCK
    slots = arrived_ref.shape[0]
    components = packed_ref.shape[0] // slots
    copies = [
        pltpu.make_async_copy(items_vmem, items_ref, sems.at[0]),
        pltpu.make_async_copy(camera_vmem, camera_ref, sems.at[1]),
    ]
    for copy in copies:
        copy.start()
    back_ref[...] = jnp.zeros_like(back_ref)
    for slot in range(slots):
        kept = min(ROWS, packed_ref.shape[0] - slot * components)
        arrived_ref[slot, 0:kept, :] = packed_ref[slot * components : slot * components + kept, :]
        if kept < ROWS:
            arrived_ref[slot, kept:, :] = jnp.zeros((ROWS - kept, BLOCK), f32)
    goal = jnp.concatenate([goal_ref[ch] for ch in range(channels)], axis=0)
    size = channels * tiles
    blurred_goal = precise_dot(padded_rows([goal, goal * goal]), table_ref, ((1,), (1,)))
    local_b, square_b = blurred_goal[:size], blurred_goal[size : 2 * size]
    for copy in copies:
        copy.wait()
    row8 = lax.broadcasted_iota(jnp.int32, (ROWS, BLOCK), 0)
    places = (lax.broadcasted_iota(jnp.int32, (SIDE, BLOCK), 0).astype(f32) + 0.5) / SIDE

    def forward(index, carry):
        slot = items_ref[index // tiles, index % tiles]
        raw = arrived_ref[slot]
        sig = jax.nn.sigmoid(raw)
        spread = 0.5 * jnp.exp(-2.0 * raw)
        value = jnp.where(row8 < 2, raw, jnp.where(row8 == 2, spread, jnp.where(row8 == 3, opacity_cap * sig, sig)))
        quant_ref[index] = value
        delta_x = places - value[0:1]
        delta_y = places - value[1:2]
        factor_x = jnp.exp(-(delta_x * delta_x) * value[2:3])
        factor_y = value[3:4] * jnp.exp(-(delta_y * delta_y) * value[2:3])
        colour = jnp.where(row8 == 7, 1.0, jnp.where(row8 >= 4, value, 0.0))
        high = colour.astype(bf16).astype(f32)
        low = colour - high
        left = jnp.concatenate([pltpu.roll(low, 5, 0), high + pltpu.roll(high, 4, 0)], axis=0)
        left_ref[index] = left
        left = left.astype(bf16)
        factor_x = jnp.concatenate([factor_x] * (BLOCK // SIDE), axis=0).T
        prods, rights = [], []
        for half in range(halves):
            tall = [
                jnp.broadcast_to(factor_y[half * ROWS + row : half * ROWS + row + 1], (SIDE, BLOCK)) for row in range(ROWS)
            ]
            tall = jnp.concatenate(tall, axis=0).T
            prod, highs, lows = None, [], []
            for chunk in range(BLOCK // CHUNK):
                rows = slice(chunk * CHUNK, (chunk + 1) * CHUNK)
                alpha = factor_x[rows] * tall[rows]
                alpha_ref[index, half, rows, :] = alpha
                high, low = split_pair(alpha)
                split_ref[half, pl.ds(pl.multiple_of(index * BLOCK + chunk * CHUNK, CHUNK), CHUNK), :] = high
                highs.append(high)
                lows.append(low)
                clear = 1.0 - alpha
                prod = clear if prod is None else prod * clear
            prods.append(prod)
            rights.append(jnp.concatenate(highs + lows, axis=0))
        sums = jnp.dot(
            jnp.concatenate([left, left], axis=1), jnp.concatenate(rights, axis=1), preferred_element_type=f32
        )
        sums = sums[ROWS:] + pltpu.roll(sums[:ROWS], ROWS - 1, 0)
        for half in range(halves):
            prod = prods[half][:ROWS] * prods[half][ROWS:]
            for shift in (4, 2, 1):
                prod = prod * pltpu.roll(prod, shift, 0)
            part_ref[half, pl.ds(pl.multiple_of(index * ROWS, ROWS), ROWS), :] = jnp.where(
                row8 == 4, prod, sums[:, half * BLOCK : (half + 1) * BLOCK]
            )
        return carry

    lax.fori_loop(0, count, forward, 0, unroll=UNROLL)

    def gathered(row, rank):
        rows = pl.ds(rank * tiles * ROWS + row, tiles, stride=ROWS)
        return jnp.concatenate([part_ref[half, rows, :] for half in range(halves)], axis=1)

    transmits = [gathered(4, rank) for rank in range(depth)]
    totals = [gathered(3, rank) for rank in range(depth)]
    floors = [jnp.maximum(total, weight_floor) for total in totals]
    ratios = [(1.0 - transmit) / floor for transmit, floor in zip(transmits, floors)]
    weighted = [[gathered(ch, rank) for ch in range(channels)] for rank in range(depth)]
    shaded = [[ratios[rank] * weighted[rank][ch] for ch in range(channels)] for rank in range(depth)]
    fronts = [jnp.ones_like(transmits[0])]
    for rank in range(depth):
        fronts.append(fronts[rank] * transmits[rank])
    images = [sum(fronts[rank] * shaded[rank][ch] for rank in range(depth)) for ch in range(channels)]
    image = jnp.concatenate(images, axis=0)
    blurred = precise_dot(padded_rows([image, image * image, image * goal]), table_ref, ((1,), (1,)))
    local_a, square_a, cross = [blurred[i * size : (i + 1) * size] for i in range(3)]
    var_a = square_a - local_a * local_a
    var_b = square_b - local_b * local_b
    both = cross - local_a * local_b
    top_one = 2.0 * local_a * local_b + stable_one
    top_two = 2.0 * both + stable_two
    low_one = local_a * local_a + local_b * local_b + stable_one
    low_two = var_a + var_b + stable_two
    under = 1.0 / (low_one * low_two)
    similar = top_one * top_two * under
    residue = image - goal
    values = (1.0 - ssim_weight) * residue * residue + ssim_weight * (1.0 - similar)
    per_tile = values[:tiles]
    for ch in range(1, channels):
        per_tile = per_tile + values[ch * tiles : (ch + 1) * tiles]
    norm = 1.0 / (channels * PIX)
    column = jnp.sum(per_tile, axis=1, keepdims=True) * norm
    loss_ref[...] = jnp.broadcast_to(column, (tiles, BLOCK)).T[0:1, :]
    loss_copy = pltpu.make_async_copy(loss_ref, loss_hbm, sems.at[2])
    loss_copy.start()
    scale = -ssim_weight * norm
    by_top_one = scale * top_two * under
    by_top_two = scale * top_one * under
    by_low_one = -scale * similar / low_one
    by_low_two = -scale * similar / low_two
    by_local = 2.0 * (local_b * (by_top_one - by_top_two) + local_a * (by_low_one - by_low_two))
    spread = precise_dot(padded_rows([by_local, by_low_two, 2.0 * by_top_two]), table_ref, ((1,), (0,)))
    by_image = (
        (2.0 * (1.0 - ssim_weight) * norm) * residue
        + spread[:size] + 2.0 * image * spread[size : 2 * size] + goal * spread[2 * size : 3 * size]
    )
    by_image = [by_image[ch * tiles : (ch + 1) * tiles] for ch in range(channels)]
    diff_ref[...] = jnp.zeros_like(diff_ref)

    def spread_rows(row, rank, value):
        rows = pl.ds(rank * tiles * 2 * ROWS + row, tiles, stride=2 * ROWS)
        for half in range(halves):
            diff_ref[half, rows, :] = value[:, half * BLOCK : (half + 1) * BLOCK]

    by_front = None
    for rank in reversed(range(depth)):
        by_shaded = [fronts[rank] * by_image[ch] for ch in range(channels)]
        by_transmit = -sum(by_shaded[ch] * weighted[rank][ch] for ch in range(channels)) / floors[rank]
        if by_front is not None:
            by_transmit = by_transmit + by_front * fronts[rank]
        own = sum(by_image[ch] * shaded[rank][ch] for ch in range(channels))
        by_front = own if by_front is None else own + by_front * transmits[rank]
        by_floor = -sum(by_shaded[ch] * shaded[rank][ch] for ch in range(channels)) / floors[rank]
        total = totals[rank]
        by_total = by_floor * jnp.where(total > weight_floor, 1.0, jnp.where(total == weight_floor, 0.5, 0.0))
        for q in range(4):
            value = by_shaded[q] * ratios[rank] if q < channels else by_total
            high = value.astype(bf16).astype(f32)
            spread_rows(8 + q, rank, high)
            spread_rows(12 + q, rank, value - high)
            if q < channels:
                spread_rows(1 + q, rank, high)
        spread_rows(0, rank, by_transmit * transmits[rank])

    xx = 1.0 + camera_ref[0, 0]
    xy = camera_ref[0, 1]
    yx = camera_ref[0, 2]
    yy = 1.0 + camera_ref[0, 3]

    group = BLOCK // (2 * ROWS)
    span = group * BLOCK
    places = lax.broadcasted_iota(jnp.int32, (BLOCK, PIX), 1)
    column = lax.broadcasted_iota(jnp.int32, (BLOCK, PIX), 0)
    middle = (SIDE - 1) / 2
    cell_x = (places % SIDE).astype(f32) - middle
    cell_y = (places // SIDE).astype(f32) - middle
    basis = jnp.where(column == ROWS // 2, 1.0, 0.0)
    for free, value in zip((5, 6, 7, 20), (cell_x, cell_y, cell_x * cell_x, cell_y * cell_y)):
        basis = jnp.where(column == free, value, basis)
    basis = basis.astype(bf16)
    basis = jnp.concatenate([basis, basis], axis=1)
    contract = (((1,), (1,)), ((), ()))

    owner_lane = lax.broadcasted_iota(jnp.int32, (BLOCK, BLOCK), 1) // (2 * ROWS)

    def mixed(step):
        block = pl.ds(step * BLOCK, BLOCK)
        rows = jnp.concatenate([diff_ref[half, block, :] for half in range(halves)], axis=1).astype(bf16)
        lefts = [left_ref[step * group + item] for item in range(group)]
        turned = jnp.concatenate(lefts, axis=0).T
        turned = [jnp.where(owner_lane == item, turned, 0.0).astype(bf16) for item in range(group)]
        mix = jnp.dot(jnp.concatenate(turned, axis=0), rows, preferred_element_type=f32)
        return rows, mix

    def gradients(step, mix):
        found = [[] for _ in range(2 * halves)]
        for item in range(group):
            index = step * group + item
            for half in range(halves):
                by_log = diff_ref[half, pl.ds(index * 2 * ROWS, 1), :]
                for chunk in range(BLOCK // CHUNK):
                    alpha = alpha_ref[index, half, chunk * CHUNK : (chunk + 1) * CHUNK, :]
                    inverse = 1.0 / (1.0 - alpha)
                    first = item * BLOCK + chunk * CHUNK
                    grad = alpha * (mix[first : first + CHUNK, half * BLOCK : (half + 1) * BLOCK] - by_log * inverse)
                    high, low = split_pair(grad)
                    found[half].append(high)
                    found[halves + half].append(low)
        return [jnp.concatenate(pieces, axis=0) for pieces in found]

    def moments_of(step, rows, left):
        wide = pl.ds(step * span, span)
        left = left + [split_ref[half, wide, :] for half in range(halves)]
        return lax.dot_general(
            jnp.concatenate(left, axis=1), jnp.concatenate([basis, rows], axis=1), contract, preferred_element_type=f32
        )

    def finished(step, totals):
        for item in range(group):
            finish(step * group + item, item, totals[item * BLOCK : (item + 1) * BLOCK].T)

    def finish(index, item, moments):
        slot = items_ref[index // tiles, index % tiles]
        value = quant_ref[index]
        inverse = value[2:3]
        base_x = 0.5 - value[0:1]
        base_y = 0.5 - value[1:2]
        zero, one_x, one_y = moments[4:5], moments[5:6] * (1.0 / SIDE), moments[6:7] * (1.0 / SIDE)
        two = (moments[7:8] + moments[20:21]) * (1.0 / (SIDE * SIDE))
        sum_x = one_x + base_x * zero
        sum_y = one_y + base_y * zero
        sum_r = two + 2.0 * (base_x * one_x + base_y * one_y) + (base_x * base_x + base_y * base_y) * zero
        by_u = 2.0 * inverse * sum_x
        by_w = 2.0 * inverse * sum_y
        back_ref[slot, 0:1, :] = xx * by_u + yx * by_w
        back_ref[slot, 1:2, :] = xy * by_u + yy * by_w
        back_ref[slot, 2:3, :] = 2.0 * inverse * sum_r
        back_ref[slot, 3:4, :] = zero * (1.0 - value[3:4] * (1.0 / opacity_cap))
        shade = value[4:7]
        first = item * 2 * ROWS + ROWS
        back_ref[slot, 4:7, :] = (moments[first : first + 3] + moments[first + 4 : first + 7]) * shade * (1.0 - shade)

    steps = count // group
    rows = [mixed(0)]
    waiting = None
    for step in range(steps):
        if step + 1 < steps:
            rows.append(mixed(step + 1))
        totals = moments_of(step, rows[step][0], gradients(step, rows[step][1]))
        if waiting is not None:
            finished(step - 1, waiting)
        waiting = totals
    finished(steps - 1, waiting)
    for slot in range(slots):
        packed_back_ref[slot * components : (slot + 1) * components, :] = back_ref[slot, 0:components, :]
    loss_copy.wait()


def scatter_kernel(ids_ref, grads_ref, out_ref):
    lanes = ids_ref.shape[1]
    components = PARAMS
    slots = grads_ref.shape[0] // components
    blocks = out_ref.shape[0] // components
    block = lax.broadcasted_iota(jnp.int32, (blocks, lanes), 0)
    chosen = jnp.where(block == ids_ref[0:1, :], 1.0, 0.0).astype(bf16)
    columns = []
    for row in range(components):
        rest, parts = grads_ref[pl.ds(row, slots, stride=components), :], []
        for _ in range(3):
            parts.append(rest.astype(bf16))
            rest = rest - parts[-1].astype(f32)
        if lanes > 3 * slots:
            parts.append(jnp.zeros((lanes - 3 * slots, BLOCK), bf16))
        columns.append(jnp.concatenate(parts, axis=0))
    sums = jnp.dot(chosen, jnp.concatenate(columns, axis=1), preferred_element_type=f32)
    for row in range(components):
        out_ref[pl.ds(row, blocks, stride=components), :] = sums[:, row * BLOCK : (row + 1) * BLOCK]


def adam_kernel(own_ref, other_ref, params_ref, one_ref, two_ref, out_hbm, out_ref, sems):
    fix_one = 1.0 - beta_one**first_step
    fix_two = 1.0 - beta_two**first_step
    components = params_ref.shape[0]
    chunks = sems.shape[0]
    width = params_ref.shape[1] // chunks
    copies = []
    for chunk in range(chunks):
        for block in range(chunk * width // BLOCK, (chunk + 1) * width // BLOCK):
            lanes = pl.ds(block * BLOCK, BLOCK)
            rows = slice(block * components, (block + 1) * components)
            grad = own_ref[rows, :]
            if other_ref is not None:
                grad = grad + other_ref[rows, :]
            one = beta_one * one_ref[:, lanes] + (1.0 - beta_one) * grad
            two = beta_two * two_ref[:, lanes] + (1.0 - beta_two) * grad * grad
            out_ref[:, lanes] = params_ref[:, lanes] - learn_rate * (one / fix_one) / (
                jnp.sqrt(two / fix_two) + adam_eps
            )
        lanes = pl.ds(chunk * width, width)
        copies.append(pltpu.make_async_copy(out_ref.at[:, lanes], out_hbm.at[:, lanes], sems.at[chunk]))
        copies[-1].start()
    for copy in copies:
        copy.wait()


def limit(size):
    return pltpu.CompilerParams(vmem_limit_bytes=size * 1024 * 1024)


def shards(params, first_moment, second_moment, camera, slot_block, slot_anchor, tile_items, target):
    cells = lax.axis_size("cell")
    views = lax.axis_size("view")
    capacity = slot_block.shape[-1]
    tiles, depth = tile_items.shape[2:]
    channels = target.shape[3]
    per_cell = params.shape[1]
    blocks = per_cell // BLOCK
    slots = cells * capacity
    count = tiles * depth
    halves = PIX // BLOCK

    camera_row = camera.reshape(1, 4)
    block_ids = jnp.swapaxes(slot_block, 3, 4).reshape(capacity, cells)
    anchors = jnp.swapaxes(slot_anchor, 4, 5).reshape(2, capacity, cells)
    items = jnp.swapaxes(tile_items, 2, 3).reshape(depth, tiles)
    goals = jnp.transpose(target, (0, 1, 3, 2, 4)).reshape(channels, tiles, PIX)
    slab = jax.ShapeDtypeStruct((slots * PARAMS, BLOCK), f32)
    id_lanes = -(-3 * slots // BLOCK) * BLOCK

    def exchange(array):
        array = array.reshape(cells, 1, capacity * PARAMS * BLOCK)
        array = lax.all_to_all(array, "cell", split_axis=0, concat_axis=0, tiled=True)
        return array.reshape(slots * PARAMS, BLOCK)

    packed, items, camera_row, ids = pl.pallas_call(
        pack_kernel,
        out_shape=(slab, jax.ShapeDtypeStruct(items.shape, items.dtype), jax.ShapeDtypeStruct(camera_row.shape, f32),
                   jax.ShapeDtypeStruct((ROWS, id_lanes), jnp.int32)),
        in_specs=[hbm] * 5,
        out_specs=(vmem,) * 4,
        scratch_shapes=[
            pltpu.SMEM(block_ids.shape, jnp.int32),
            pltpu.SMEM(anchors.shape, f32),
            pltpu.SMEM(camera_row.shape, f32),
            pltpu.VMEM(params.shape, f32),
            pltpu.SemaphoreType.DMA((6,)),
        ],
        compiler_params=limit(4),
        name="pack",
    )(*[pltpu.with_memory_space_constraint(array, pltpu.HBM) for array in (block_ids, anchors, camera_row, params, items)])
    arrived = exchange(packed)
    back, losses = pl.pallas_call(
        owner_kernel,
        out_shape=(slab, jax.ShapeDtypeStruct((1, tiles), f32)),
        in_specs=[vmem] * 5,
        out_specs=(vmem, hbm),
        scratch_shapes=[
            pltpu.SMEM(items.shape, jnp.int32),
            pltpu.SMEM(camera_row.shape, f32),
            pltpu.VMEM((1, tiles), f32),
            pltpu.SemaphoreType.DMA((3,)),
            pltpu.VMEM((slots, ROWS, BLOCK), f32),
            pltpu.VMEM((slots, ROWS, BLOCK), f32),
            pltpu.VMEM((count, ROWS, BLOCK), f32),
            pltpu.VMEM((count, 2 * ROWS, BLOCK), f32),
            pltpu.VMEM((count, halves, BLOCK, BLOCK), f32),
            pltpu.VMEM((halves, count * BLOCK, BLOCK), bf16),
            pltpu.VMEM((halves, count * ROWS, BLOCK), f32),
            pltpu.VMEM((halves, count * 2 * ROWS, BLOCK), f32),
        ],
        compiler_params=limit(40),
        name="owner",
    )(items, camera_row, arrived, goals, jnp.asarray(blur_kron()))
    returned = exchange(back)
    summed = pl.pallas_call(
        scatter_kernel,
        out_shape=jax.ShapeDtypeStruct((blocks * PARAMS, BLOCK), f32),
        in_specs=[vmem, vmem],
        out_specs=vmem,
        compiler_params=limit(4),
        name="scatter",
    )(ids, returned)
    operands = [summed]
    body = adam_kernel
    if views == 2:
        operands.append(lax.ppermute(summed, "view", [(0, 1), (1, 0)]))
    else:
        operands = [lax.psum(summed, "view")]
        body = lambda own, *rest: adam_kernel(own, None, *rest)
    current = pl.pallas_call(
        body,
        out_shape=jax.ShapeDtypeStruct(params.shape, f32),
        in_specs=[vmem] * (len(operands) + 3),
        out_specs=hbm,
        scratch_shapes=[pltpu.VMEM(params.shape, f32), pltpu.SemaphoreType.DMA((4,))],
        compiler_params=limit(4),
        name="adam",
    )(*operands, params, first_moment, second_moment)
    return current, losses.reshape(1, 1, tiles)


def solution(mesh):
    placed = (
        P(None, "cell"),
        P(None, "cell"),
        P(None, "cell"),
        P(None, "view", None),
        P(None, "view", "cell", None, None),
        P(None, "view", "cell", None, None, None),
        P(None, "view", "cell", None),
        P(None, "view", "cell", None, None),
    )
    return jax.shard_map(
        shards,
        mesh=mesh,
        in_specs=placed,
        out_specs=(P(None, "cell"), P(None, "view", "cell")),
        check_vma=False,
    )
```

```python
import functools

import jax
import jax.numpy as jnp
import numpy as np
from jax import lax
from jax.experimental import pallas as pl
from jax.experimental.pallas import tpu as pltpu
from jax.sharding import PartitionSpec as P

SIDE = 16
BLOCK = 128
TAPS = 11
PIX = SIDE * SIDE
ROWS = 8
PARAMS = 7

ssim_weight = 0.2
stable_one = 0.0001
stable_two = 0.0009
learn_rate = 0.1
beta_one = 0.9
beta_two = 0.999
adam_eps = 1e-08
first_step = 1
opacity_cap = 0.1
weight_floor = 0.5
f32 = jnp.float32
bf16 = jnp.bfloat16
CHUNK = 16
UNROLL = 32

vmem = pl.BlockSpec(memory_space=pltpu.VMEM)
hbm = pl.BlockSpec(memory_space=pltpu.HBM)


def blur_kron():
    offsets = np.arange(SIDE)[:, None] - np.arange(SIDE)[None, :]
    kernel = np.exp(-(offsets * offsets) / 4.5) * (np.abs(offsets) <= TAPS // 2)
    kernel = kernel / kernel.sum(axis=1, keepdims=True)
    table, parts = np.kron(kernel, kernel).astype(np.float32), []
    for _ in range(3):
        parts.append(table.astype(bf16))
        table = table - parts[-1].astype(np.float32)
    return np.stack(parts)


def pack_kernel(
    block_hbm, anchor_hbm, camera_hbm, params_hbm, items_hbm,
    out_ref, items_ref, row_ref, ids_ref,
    block_ref, anchor_ref, camera_ref, params_ref, sems,
):
    capacity, owners = block_ref.shape
    components = params_ref.shape[0]
    pairs = (
        (params_hbm, params_ref), (block_hbm, block_ref), (anchor_hbm, anchor_ref), (camera_hbm, camera_ref),
        (items_hbm, items_ref), (camera_hbm, row_ref),
    )
    copies = [pltpu.make_async_copy(source, target, sems.at[i]) for i, (source, target) in enumerate(pairs)]
    for copy in copies:
        copy.start()
    for copy in copies[1:]:
        copy.wait()
    xx = 1.0 + camera_ref[0, 0]
    xy = camera_ref[0, 1]
    yx = camera_ref[0, 2]
    yy = 1.0 + camera_ref[0, 3]
    slots = owners * capacity
    lane = lax.broadcasted_iota(jnp.int32, ids_ref.shape, 1)
    lane = jnp.where(lane < 3 * slots, lane % slots, -1)
    ids = jnp.full(ids_ref.shape, -1, jnp.int32)
    for index in range(slots):
        ids = jnp.where(lane == index, block_ref[index % capacity, index // capacity], ids)
    ids_ref[...] = ids
    copies[0].wait()
    for index in range(slots):
        owner, slot = index // capacity, index % capacity
        block = block_ref[slot, owner]
        lanes = pl.ds(pl.multiple_of(jnp.maximum(block, 0) * BLOCK, BLOCK), BLOCK)
        tile = params_ref[:, lanes]
        pos_x, pos_y = tile[0:1], tile[1:2]
        row = index * components
        out_ref[row : row + 1, :] = xx * pos_x + xy * pos_y + anchor_ref[0, slot, owner]
        out_ref[row + 1 : row + 2, :] = yx * pos_x + yy * pos_y + anchor_ref[1, slot, owner]
        out_ref[row + 2 : row + components, :] = tile[2:]


def split_pair(value):
    high = value.astype(bf16)
    return high, (value - high.astype(f32)).astype(bf16)


def precise_dot(value, table_ref, dims):
    rows = value.shape[0]
    parts, rest = [], value
    for _ in range(3):
        parts.append(rest.astype(bf16))
        rest = rest - parts[-1].astype(f32)
    total = None
    for index in range(3):
        left = jnp.concatenate(parts[: 3 - index], axis=0)
        product = lax.dot_general(left, table_ref[index], (dims, ((), ())), preferred_element_type=f32)
        for part in range(3 - index):
            piece = product[part * rows : (part + 1) * rows]
            total = piece if total is None else total + piece
    return total


def padded_rows(values):
    rows = sum(value.shape[0] for value in values)
    extra = -rows % (2 * ROWS)
    if extra:
        values = values + [jnp.zeros((extra, values[0].shape[1]), f32)]
    return jnp.concatenate(values, axis=0)


def owner_kernel(
    items_vmem, camera_vmem, packed_ref, goal_ref, table_ref,
    packed_back_ref, loss_hbm,
    items_ref, camera_ref, loss_ref, sems, arrived_ref, back_ref, quant_ref, left_ref, alpha_ref, split_ref, part_ref, diff_ref,
):
    depth, tiles = items_ref.shape
    channels = goal_ref.shape[0]
    count = depth * tiles
    halves = PIX // BLOCK
    slots = arrived_ref.shape[0]
    components = packed_ref.shape[0] // slots
    copies = [
        pltpu.make_async_copy(items_vmem, items_ref, sems.at[0]),
        pltpu.make_async_copy(camera_vmem, camera_ref, sems.at[1]),
    ]
    for copy in copies:
        copy.start()
    back_ref[...] = jnp.zeros_like(back_ref)
    row8 = lax.broadcasted_iota(jnp.int32, (ROWS, BLOCK), 0)
    for slot in range(slots):
        kept = min(ROWS, packed_ref.shape[0] - slot * components)
        arrived_ref[slot, 0:kept, :] = packed_ref[slot * components : slot * components + kept, :]
        if kept < ROWS:
            arrived_ref[slot, kept:, :] = jnp.zeros((ROWS - kept, BLOCK), f32)
        raw = arrived_ref[slot]
        sig = jax.nn.sigmoid(raw)
        spread = 0.5 * jnp.exp(-2.0 * raw)
        arrived_ref[slot] = jnp.where(row8 < 2, raw, jnp.where(row8 == 2, spread, jnp.where(row8 == 3, opacity_cap * sig, sig)))
    goal = jnp.concatenate([goal_ref[ch] for ch in range(channels)], axis=0)
    size = channels * tiles
    blurred_goal = precise_dot(padded_rows([goal, goal * goal]), table_ref, ((1,), (1,)))
    local_b, square_b = blurred_goal[:size], blurred_goal[size : 2 * size]
    for copy in copies:
        copy.wait()
    places = (lax.broadcasted_iota(jnp.int32, (SIDE, BLOCK), 0).astype(f32) + 0.5) / SIDE

    def forward(index, carry):
        slot = items_ref[index // tiles, index % tiles]
        value = arrived_ref[slot]
        quant_ref[index] = value
        delta_x = places - value[0:1]
        delta_y = places - value[1:2]
        factor_x = jnp.exp(-(delta_x * delta_x) * value[2:3])
        factor_y = value[3:4] * jnp.exp(-(delta_y * delta_y) * value[2:3])
        colour = jnp.where(row8 == 7, 1.0, jnp.where(row8 >= 4, value, 0.0))
        high = colour.astype(bf16).astype(f32)
        low = colour - high
        left = jnp.concatenate([pltpu.roll(low, 5, 0), high + pltpu.roll(high, 4, 0)], axis=0)
        left_ref[index] = left
        left = left.astype(bf16)
        factor_x = jnp.concatenate([factor_x] * (BLOCK // SIDE), axis=0).T
        prods, rights = [], []
        for half in range(halves):
            tall = [
                jnp.broadcast_to(factor_y[half * ROWS + row : half * ROWS + row + 1], (SIDE, BLOCK)) for row in range(ROWS)
            ]
            tall = jnp.concatenate(tall, axis=0).T
            prod, highs, lows = None, [], []
            for chunk in range(BLOCK // CHUNK):
                rows = slice(chunk * CHUNK, (chunk + 1) * CHUNK)
                alpha = factor_x[rows] * tall[rows]
                alpha_ref[index, half, rows, :] = alpha
                high, low = split_pair(alpha)
                split_ref[half, pl.ds(pl.multiple_of(index * BLOCK + chunk * CHUNK, CHUNK), CHUNK), :] = high
                highs.append(high)
                lows.append(low)
                clear = 1.0 - alpha
                prod = clear if prod is None else prod * clear
            prods.append(prod)
            rights.append(jnp.concatenate(highs + lows, axis=0))
        sums = jnp.dot(
            jnp.concatenate([left, left], axis=1), jnp.concatenate(rights, axis=1), preferred_element_type=f32
        )
        sums = sums[ROWS:] + pltpu.roll(sums[:ROWS], ROWS - 1, 0)
        for half in range(halves):
            prod = prods[half][:ROWS] * prods[half][ROWS:]
            for shift in (4, 2, 1):
                prod = prod * pltpu.roll(prod, shift, 0)
            part_ref[half, pl.ds(pl.multiple_of(index * ROWS, ROWS), ROWS), :] = jnp.where(
                row8 == 4, prod, sums[:, half * BLOCK : (half + 1) * BLOCK]
            )
        return carry

    lax.fori_loop(0, count, forward, 0, unroll=UNROLL)

    def gathered(row, rank):
        rows = pl.ds(rank * tiles * ROWS + row, tiles, stride=ROWS)
        return jnp.concatenate([part_ref[half, rows, :] for half in range(halves)], axis=1)

    transmits = [gathered(4, rank) for rank in range(depth)]
    totals = [gathered(3, rank) for rank in range(depth)]
    floors = [jnp.maximum(total, weight_floor) for total in totals]
    ratios = [(1.0 - transmit) / floor for transmit, floor in zip(transmits, floors)]
    weighted = [[gathered(ch, rank) for ch in range(channels)] for rank in range(depth)]
    shaded = [[ratios[rank] * weighted[rank][ch] for ch in range(channels)] for rank in range(depth)]
    fronts = [jnp.ones_like(transmits[0])]
    for rank in range(depth):
        fronts.append(fronts[rank] * transmits[rank])
    images = [sum(fronts[rank] * shaded[rank][ch] for rank in range(depth)) for ch in range(channels)]
    image = jnp.concatenate(images, axis=0)
    blurred = precise_dot(padded_rows([image, image * image, image * goal]), table_ref, ((1,), (1,)))
    local_a, square_a, cross = [blurred[i * size : (i + 1) * size] for i in range(3)]
    var_a = square_a - local_a * local_a
    var_b = square_b - local_b * local_b
    both = cross - local_a * local_b
    top_one = 2.0 * local_a * local_b + stable_one
    top_two = 2.0 * both + stable_two
    low_one = local_a * local_a + local_b * local_b + stable_one
    low_two = var_a + var_b + stable_two
    under = 1.0 / (low_one * low_two)
    similar = top_one * top_two * under
    residue = image - goal
    values = (1.0 - ssim_weight) * residue * residue + ssim_weight * (1.0 - similar)
    per_tile = values[:tiles]
    for ch in range(1, channels):
        per_tile = per_tile + values[ch * tiles : (ch + 1) * tiles]
    norm = 1.0 / (channels * PIX)
    column = jnp.sum(per_tile, axis=1, keepdims=True) * norm
    loss_ref[...] = jnp.broadcast_to(column, (tiles, BLOCK)).T[0:1, :]
    loss_copy = pltpu.make_async_copy(loss_ref, loss_hbm, sems.at[2])
    loss_copy.start()
    scale = -ssim_weight * norm
    by_top_one = scale * top_two * under
    by_top_two = scale * top_one * under
    by_low_one = -scale * similar / low_one
    by_low_two = -scale * similar / low_two
    by_local = 2.0 * (local_b * (by_top_one - by_top_two) + local_a * (by_low_one - by_low_two))
    spread = precise_dot(padded_rows([by_local, by_low_two, 2.0 * by_top_two]), table_ref, ((1,), (0,)))
    by_image = (
        (2.0 * (1.0 - ssim_weight) * norm) * residue
        + spread[:size] + 2.0 * image * spread[size : 2 * size] + goal * spread[2 * size : 3 * size]
    )
    by_image = [by_image[ch * tiles : (ch + 1) * tiles] for ch in range(channels)]
    diff_ref[...] = jnp.zeros_like(diff_ref)

    def spread_rows(row, rank, value):
        rows = pl.ds(rank * tiles * 2 * ROWS + row, tiles, stride=2 * ROWS)
        for half in range(halves):
            diff_ref[half, rows, :] = value[:, half * BLOCK : (half + 1) * BLOCK]

    by_front = None
    for rank in reversed(range(depth)):
        by_shaded = [fronts[rank] * by_image[ch] for ch in range(channels)]
        by_transmit = -sum(by_shaded[ch] * weighted[rank][ch] for ch in range(channels)) / floors[rank]
        if by_front is not None:
            by_transmit = by_transmit + by_front * fronts[rank]
        own = sum(by_image[ch] * shaded[rank][ch] for ch in range(channels))
        by_front = own if by_front is None else own + by_front * transmits[rank]
        by_floor = -sum(by_shaded[ch] * shaded[rank][ch] for ch in range(channels)) / floors[rank]
        total = totals[rank]
        by_total = by_floor * jnp.where(total > weight_floor, 1.0, jnp.where(total == weight_floor, 0.5, 0.0))
        for q in range(4):
            value = by_shaded[q] * ratios[rank] if q < channels else by_total
            high = value.astype(bf16).astype(f32)
            spread_rows(8 + q, rank, high)
            spread_rows(12 + q, rank, value - high)
            if q < channels:
                spread_rows(1 + q, rank, high)
        spread_rows(0, rank, by_transmit * transmits[rank])

    xx = 1.0 + camera_ref[0, 0]
    xy = camera_ref[0, 1]
    yx = camera_ref[0, 2]
    yy = 1.0 + camera_ref[0, 3]

    group = BLOCK // (2 * ROWS)
    span = group * BLOCK
    places = lax.broadcasted_iota(jnp.int32, (BLOCK, PIX), 1)
    column = lax.broadcasted_iota(jnp.int32, (BLOCK, PIX), 0)
    middle = (SIDE - 1) / 2
    cell_x = (places % SIDE).astype(f32) - middle
    cell_y = (places // SIDE).astype(f32) - middle
    basis = jnp.where(column == ROWS // 2, 1.0, 0.0)
    for free, value in zip((5, 6, 7, 20), (cell_x, cell_y, cell_x * cell_x, cell_y * cell_y)):
        basis = jnp.where(column == free, value, basis)
    basis = basis.astype(bf16)
    basis = jnp.concatenate([basis, basis], axis=1)
    contract = (((1,), (1,)), ((), ()))

    owner_lane = lax.broadcasted_iota(jnp.int32, (BLOCK, BLOCK), 1) // (2 * ROWS)

    def mixed(step):
        block = pl.ds(step * BLOCK, BLOCK)
        rows = jnp.concatenate([diff_ref[half, block, :] for half in range(halves)], axis=1).astype(bf16)
        lefts = [left_ref[step * group + item] for item in range(group)]
        turned = jnp.concatenate(lefts, axis=0).T
        turned = [jnp.where(owner_lane == item, turned, 0.0).astype(bf16) for item in range(group)]
        mix = jnp.dot(jnp.concatenate(turned, axis=0), rows, preferred_element_type=f32)
        return rows, mix

    def gradients(step, mix):
        found = [[] for _ in range(2 * halves)]
        for item in range(group):
            index = step * group + item
            for half in range(halves):
                by_log = diff_ref[half, pl.ds(index * 2 * ROWS, 1), :]
                for chunk in range(BLOCK // CHUNK):
                    alpha = alpha_ref[index, half, chunk * CHUNK : (chunk + 1) * CHUNK, :]
                    inverse = 1.0 / (1.0 - alpha)
                    first = item * BLOCK + chunk * CHUNK
                    grad = alpha * (mix[first : first + CHUNK, half * BLOCK : (half + 1) * BLOCK] - by_log * inverse)
                    high, low = split_pair(grad)
                    found[half].append(high)
                    found[halves + half].append(low)
        return [jnp.concatenate(pieces, axis=0) for pieces in found]

    def moments_of(step, rows, left):
        wide = pl.ds(step * span, span)
        left = left + [split_ref[half, wide, :] for half in range(halves)]
        return lax.dot_general(
            jnp.concatenate(left, axis=1), jnp.concatenate([basis, rows], axis=1), contract, preferred_element_type=f32
        )

    def finished(step, totals):
        for item in range(group):
            finish(step * group + item, item, totals[item * BLOCK : (item + 1) * BLOCK].T)

    def finish(index, item, moments):
        slot = items_ref[index // tiles, index % tiles]
        value = quant_ref[index]
        inverse = value[2:3]
        base_x = 0.5 - value[0:1]
        base_y = 0.5 - value[1:2]
        zero, one_x, one_y = moments[4:5], moments[5:6] * (1.0 / SIDE), moments[6:7] * (1.0 / SIDE)
        two = (moments[7:8] + moments[20:21]) * (1.0 / (SIDE * SIDE))
        sum_x = one_x + base_x * zero
        sum_y = one_y + base_y * zero
        sum_r = two + 2.0 * (base_x * one_x + base_y * one_y) + (base_x * base_x + base_y * base_y) * zero
        by_u = 2.0 * inverse * sum_x
        by_w = 2.0 * inverse * sum_y
        back_ref[slot, 0:1, :] = xx * by_u + yx * by_w
        back_ref[slot, 1:2, :] = xy * by_u + yy * by_w
        back_ref[slot, 2:3, :] = 2.0 * inverse * sum_r
        back_ref[slot, 3:4, :] = zero * (1.0 - value[3:4] * (1.0 / opacity_cap))
        shade = value[4:7]
        first = item * 2 * ROWS + ROWS
        back_ref[slot, 4:7, :] = (moments[first : first + 3] + moments[first + 4 : first + 7]) * shade * (1.0 - shade)

    steps = count // group
    rows = [mixed(0)]
    waiting = None
    for step in range(steps):
        if step + 1 < steps:
            rows.append(mixed(step + 1))
        totals = moments_of(step, rows[step][0], gradients(step, rows[step][1]))
        if waiting is not None:
            finished(step - 1, waiting)
        waiting = totals
    finished(steps - 1, waiting)
    for slot in range(slots):
        packed_back_ref[slot * components : (slot + 1) * components, :] = back_ref[slot, 0:components, :]
    loss_copy.wait()


def scatter_kernel(ids_ref, grads_ref, out_ref):
    lanes = ids_ref.shape[1]
    components = PARAMS
    slots = grads_ref.shape[0] // components
    blocks = out_ref.shape[0] // components
    block = lax.broadcasted_iota(jnp.int32, (blocks, lanes), 0)
    chosen = jnp.where(block == ids_ref[0:1, :], 1.0, 0.0).astype(bf16)
    columns = []
    for row in range(components):
        rest, parts = grads_ref[pl.ds(row, slots, stride=components), :], []
        for _ in range(3):
            parts.append(rest.astype(bf16))
            rest = rest - parts[-1].astype(f32)
        if lanes > 3 * slots:
            parts.append(jnp.zeros((lanes - 3 * slots, BLOCK), bf16))
        columns.append(jnp.concatenate(parts, axis=0))
    sums = jnp.dot(chosen, jnp.concatenate(columns, axis=1), preferred_element_type=f32)
    for row in range(components):
        out_ref[pl.ds(row, blocks, stride=components), :] = sums[:, row * BLOCK : (row + 1) * BLOCK]


def adam_kernel(own_ref, other_ref, params_ref, one_ref, two_ref, out_hbm, out_ref, sems):
    fix_one = 1.0 - beta_one**first_step
    fix_two = 1.0 - beta_two**first_step
    components = params_ref.shape[0]
    chunks = sems.shape[0]
    width = params_ref.shape[1] // chunks
    copies = []
    for chunk in range(chunks):
        for block in range(chunk * width // BLOCK, (chunk + 1) * width // BLOCK):
            lanes = pl.ds(block * BLOCK, BLOCK)
            rows = slice(block * components, (block + 1) * components)
            grad = own_ref[rows, :]
            if other_ref is not None:
                grad = grad + other_ref[rows, :]
            one = beta_one * one_ref[:, lanes] + (1.0 - beta_one) * grad
            two = beta_two * two_ref[:, lanes] + (1.0 - beta_two) * grad * grad
            out_ref[:, lanes] = params_ref[:, lanes] - learn_rate * (one / fix_one) / (
                jnp.sqrt(two / fix_two) + adam_eps
            )
        lanes = pl.ds(chunk * width, width)
        copies.append(pltpu.make_async_copy(out_ref.at[:, lanes], out_hbm.at[:, lanes], sems.at[chunk]))
        copies[-1].start()
    for copy in copies:
        copy.wait()


def limit(size):
    return pltpu.CompilerParams(vmem_limit_bytes=size * 1024 * 1024)


def shards(params, first_moment, second_moment, camera, slot_block, slot_anchor, tile_items, target):
    cells = lax.axis_size("cell")
    views = lax.axis_size("view")
    capacity = slot_block.shape[-1]
    tiles, depth = tile_items.shape[2:]
    channels = target.shape[3]
    per_cell = params.shape[1]
    blocks = per_cell // BLOCK
    slots = cells * capacity
    count = tiles * depth
    halves = PIX // BLOCK

    camera_row = camera.reshape(1, 4)
    block_ids = jnp.swapaxes(slot_block, 3, 4).reshape(capacity, cells)
    anchors = jnp.swapaxes(slot_anchor, 4, 5).reshape(2, capacity, cells)
    items = jnp.swapaxes(tile_items, 2, 3).reshape(depth, tiles)
    goals = jnp.transpose(target, (0, 1, 3, 2, 4)).reshape(channels, tiles, PIX)
    slab = jax.ShapeDtypeStruct((slots * PARAMS, BLOCK), f32)
    id_lanes = -(-3 * slots // BLOCK) * BLOCK

    def exchange(array):
        array = array.reshape(cells, 1, capacity * PARAMS * BLOCK)
        array = lax.all_to_all(array, "cell", split_axis=0, concat_axis=0, tiled=True)
        return array.reshape(slots * PARAMS, BLOCK)

    packed, items, camera_row, ids = pl.pallas_call(
        pack_kernel,
        out_shape=(slab, jax.ShapeDtypeStruct(items.shape, items.dtype), jax.ShapeDtypeStruct(camera_row.shape, f32),
                   jax.ShapeDtypeStruct((ROWS, id_lanes), jnp.int32)),
        in_specs=[hbm] * 5,
        out_specs=(vmem,) * 4,
        scratch_shapes=[
            pltpu.SMEM(block_ids.shape, jnp.int32),
            pltpu.SMEM(anchors.shape, f32),
            pltpu.SMEM(camera_row.shape, f32),
            pltpu.VMEM(params.shape, f32),
            pltpu.SemaphoreType.DMA((6,)),
        ],
        compiler_params=limit(4),
        name="pack",
    )(*[pltpu.with_memory_space_constraint(array, pltpu.HBM) for array in (block_ids, anchors, camera_row, params, items)])
    arrived = exchange(packed)
    back, losses = pl.pallas_call(
        owner_kernel,
        out_shape=(slab, jax.ShapeDtypeStruct((1, tiles), f32)),
        in_specs=[vmem] * 5,
        out_specs=(vmem, hbm),
        scratch_shapes=[
            pltpu.SMEM(items.shape, jnp.int32),
            pltpu.SMEM(camera_row.shape, f32),
            pltpu.VMEM((1, tiles), f32),
            pltpu.SemaphoreType.DMA((3,)),
            pltpu.VMEM((slots, ROWS, BLOCK), f32),
            pltpu.VMEM((slots, ROWS, BLOCK), f32),
            pltpu.VMEM((count, ROWS, BLOCK), f32),
            pltpu.VMEM((count, 2 * ROWS, BLOCK), f32),
            pltpu.VMEM((count, halves, BLOCK, BLOCK), f32),
            pltpu.VMEM((halves, count * BLOCK, BLOCK), bf16),
            pltpu.VMEM((halves, count * ROWS, BLOCK), f32),
            pltpu.VMEM((halves, count * 2 * ROWS, BLOCK), f32),
        ],
        compiler_params=limit(40),
        name="owner",
    )(items, camera_row, arrived, goals, jnp.asarray(blur_kron()))
    returned = exchange(back)
    summed = pl.pallas_call(
        scatter_kernel,
        out_shape=jax.ShapeDtypeStruct((blocks * PARAMS, BLOCK), f32),
        in_specs=[vmem, vmem],
        out_specs=vmem,
        compiler_params=limit(4),
        name="scatter",
    )(ids, returned)
    operands = [summed]
    body = adam_kernel
    if views == 2:
        operands.append(lax.ppermute(summed, "view", [(0, 1), (1, 0)]))
    else:
        operands = [lax.psum(summed, "view")]
        body = lambda own, *rest: adam_kernel(own, None, *rest)
    current = pl.pallas_call(
        body,
        out_shape=jax.ShapeDtypeStruct(params.shape, f32),
        in_specs=[vmem] * (len(operands) + 3),
        out_specs=hbm,
        scratch_shapes=[pltpu.VMEM(params.shape, f32), pltpu.SemaphoreType.DMA((4,))],
        compiler_params=limit(4),
        name="adam",
    )(*operands, params, first_moment, second_moment)
    return current, losses.reshape(1, 1, tiles)


def solution(mesh):
    placed = (
        P(None, "cell"),
        P(None, "cell"),
        P(None, "cell"),
        P(None, "view", None),
        P(None, "view", "cell", None, None),
        P(None, "view", "cell", None, None, None),
        P(None, "view", "cell", None),
        P(None, "view", "cell", None, None),
    )
    return jax.shard_map(
        shards,
        mesh=mesh,
        in_specs=placed,
        out_specs=(P(None, "cell"), P(None, "view", "cell")),
        check_vma=False,
    )
```
